256 devices in a mesh: rack: 8 (over x, core), chip: 32 (over y, z).
Axes of the slice: x: 4, y: 4, z: 8, core: 2. Of those that a mesh axis runs over, the one named last changes fastest.
Arguments:
- points: float32 [512, 4, 32, 256], P(('rack', 'chip')), may hold values from -6 to 6
- counts: int32 [512, 256], P(('rack', 'chip')), may hold values from 1 to 32
- cells: int32 [512, 256], P(('rack', 'chip')), may hold values from 0 to 2047, as said below
- pfn_weight: float32 [9, 64], replicated, may hold values from -2 to 2
- pfn_gain: float32 [64], replicated, may hold values from 0.5 to 1.5
- pfn_bias: float32 [64], replicated, may hold values from -3 to 3
- conv_weight: float32 [4, 9, 4096], replicated, may hold values from -0.25 to 0.25
- bn_gain: float32 [4, 64], replicated, may hold values from 0.5 to 1.5
- bn_bias: float32 [4, 64], replicated, may hold values from -3 to 3
- cotangent: float32 [512, 64, 4, 128], P(('rack', 'chip')), may hold values from -0.006 to 0.006
Outputs:
- features: float32 [512, 64, 4, 128], P(('rack', 'chip'))
- conv_grads: float32 [4, 9, 4096], replicated
- norm_grads: float32 [2, 4, 64], replicated
- pillar_grad: float32 [512, 64, 256], P(('rack', 'chip'))
The draws below stay inside these ranges and needn't reach their ends.
Inputs may be any that keep to these rules, and one draw needn't show every extreme that they name: `cells`: within one sweep no two pillars share a cell.
All inputs are finite; a program needn't handle non-finite values.
Results may differ from the reference program's by a relative error of at most 0.0003.
Values sent between devices are 32-bit elements; how exact they have to be, the bound alone decides.
A program may use at most 128 MiB of HBM per device.

```python
import jax
import jax.numpy as jnp
from jax import lax

C = 64
MAXP = 32
LAYERS = 4
GH = 8
GW = 256
PILL = 256
SWEEPS = 512


def draw_cells(key, part):
    keys = jax.random.split(key, SWEEPS)

    def one_sweep(sweep_key):
        return jax.random.permutation(sweep_key, GH * GW)[:PILL].astype(jnp.int32)
    return jax.vmap(one_sweep)(keys)


def touch_ends(values, own_key, least, largest):
    dims = values.shape
    spot = [jax.random.randint(jax.random.fold_in(own_key, axis), (), 0, dims[axis]) for axis in range(len(dims))]
    values = values.at[tuple(spot)].set(least)
    longest = dims.index(max(dims))
    spot[longest] = (spot[longest] + 1) % dims[longest]
    return values.at[tuple(spot)].set(largest)


def steps_of(rng, dims, pieces, smallest, largest):
    def one(axis_at, shards_of):
        heights = jax.random.uniform(jax.random.fold_in(jax.random.fold_in(rng, 6), axis_at), (shards_of,), jnp.float32, smallest / len(pieces), largest / len(pieces))
        return jnp.repeat(jnp.exp(heights), dims[axis_at] // shards_of).reshape((-1,) + (1,) * (len(dims) - axis_at - 1))

    level = one(*pieces[0])
    for cut in pieces[1:]:
        level = level * one(*cut)
    return level


def bell_draw(own_key, shape, spread, bound, pieces=(), kind=jnp.bfloat16):
    values = jax.random.normal(own_key, shape, jnp.float32) * spread
    if len(pieces) > 0:
        values = steps_of(own_key, shape, pieces, -0.22, 0.18) * values
    return jnp.clip(values, min=-bound, max=bound).astype(kind)


def setup_inputs(seed: int = 0) -> dict:
    streams_of = jax.random.split(jax.random.key(seed), 11)
    points = bell_draw(streams_of[0], (SWEEPS, 4, MAXP, PILL), 1.0, 6.0, ((0, 256),), jnp.float32)
    counts = touch_ends(jax.random.randint(streams_of[1], (SWEEPS, PILL), 1, MAXP + 1), jax.random.fold_in(streams_of[1], 1), 1, MAXP).astype(jnp.int32)
    cells = draw_cells(jax.random.fold_in(streams_of[10], 71), 0)
    pfn_weight = bell_draw(streams_of[3], (9, C), 9 ** -0.5, 2.0, (), jnp.float32)
    pfn_gain = jnp.clip(1.0 + 0.1 * jax.random.normal(streams_of[4], (C,), jnp.float32), 0.5, 1.5)
    pfn_bias = bell_draw(streams_of[5], (C,), 0.5, 3.0, (), jnp.float32)
    conv_weight = bell_draw(streams_of[6], (LAYERS, 9, C * C), (9 * C) ** -0.5, 0.25, (), jnp.float32)
    bn_gain = jnp.clip(1.0 + 0.1 * jax.random.normal(streams_of[7], (LAYERS, C), jnp.float32), 0.5, 1.5)
    bn_bias = bell_draw(streams_of[8], (LAYERS, C), 0.5, 3.0, (), jnp.float32)
    cotangent = bell_draw(streams_of[9], (SWEEPS, C, GH // 2, GW // 2), 0.001, 0.006, ((0, 256),), jnp.float32)
    return dict(points=points, counts=counts, cells=cells, pfn_weight=pfn_weight, pfn_gain=pfn_gain, pfn_bias=pfn_bias, conv_weight=conv_weight, bn_gain=bn_gain, bn_bias=bn_bias, cotangent=cotangent)


EPS = 1e-05
PRECISE = lax.Precision.HIGHEST

def channel_shape(vector, ndim):
    return vector.reshape((1, -1) + (1,) * (ndim - 2))

def silu_slope(pre_act):
    sigma = jax.nn.sigmoid(pre_act)
    return sigma * (1.0 + pre_act * (1.0 - sigma))

def pillar_hidden(points, counts, cells, pfn_weight):
    slot_ids = lax.broadcasted_iota(jnp.int32, (1, points.shape[2], 1), 1)
    is_valid = (slot_ids < counts[:, None, :]).astype(jnp.float32)
    point_count = counts.astype(jnp.float32)
    centroid = lax.optimization_barrier(jnp.sum(points[:, 0:3] * is_valid[:, None], axis=2)) / point_count[:, None]
    col_pos = (cells % GW).astype(jnp.float32) * (2.0 / GW) - 1.0
    row_pos = (cells // GW).astype(jnp.float32) * (2.0 / GH) - 1.0
    offsets = points[:, 0:3] - centroid[:, :, None, :]
    grid_off = jnp.stack([points[:, 0] - col_pos[:, None, :], points[:, 1] - row_pos[:, None, :]], axis=1)
    inputs = jnp.concatenate([points, offsets, grid_off], axis=1)
    hidden = jnp.einsum('fc,sfpq->scpq', pfn_weight, inputs, precision=PRECISE)
    return (hidden, is_valid)

def normalize_pillars(hidden, is_valid, mean_val, inv_std, gain, bias):
    scaled = channel_shape(gain, 4) * (hidden - channel_shape(mean_val, 4)) * channel_shape(inv_std, 4) + channel_shape(bias, 4)
    return lax.optimization_barrier(jnp.max(jnp.maximum(scaled, 0.0) * is_valid[:, None], axis=2))

def scatter_pillars(pillar, cells):
    empty = jnp.zeros((pillar.shape[1], GH * GW), pillar.dtype)
    placed = jax.vmap(lambda feature, target: empty.at[:, target].set(feature))(pillar, cells)
    return placed.reshape(pillar.shape[0], pillar.shape[1], GH, GW)

def conv_forward(activation, taps, stride):
    padded = jnp.pad(activation, ((0, 0), (0, 0), (1, 1), (1, 1)))
    height = activation.shape[2] // stride
    width = activation.shape[3] // stride
    result = jnp.zeros((activation.shape[0], C, height, width), jnp.float32)
    for row_tap in range(3):
        for col_tap in range(3):
            tap_slice = padded[:, :, row_tap:row_tap + stride * height:stride, col_tap:col_tap + stride * width:stride]
            kernel = taps[3 * row_tap + col_tap].reshape(C, C)
            result = result + jnp.einsum('oi,nihw->nohw', kernel, tap_slice, precision=PRECISE)
    return result

def conv_backward(activation, taps, grad_z, stride):
    padded = jnp.pad(activation, ((0, 0), (0, 0), (1, 1), (1, 1)))
    height = grad_z.shape[2]
    width = grad_z.shape[3]
    grad_pad = jnp.zeros(padded.shape, jnp.float32)
    tap_grads = []
    for row_tap in range(3):
        for col_tap in range(3):
            tap_slice = padded[:, :, row_tap:row_tap + stride * height:stride, col_tap:col_tap + stride * width:stride]
            tap_grads.append(jnp.einsum('nohw,nihw->oi', grad_z, tap_slice, precision=PRECISE).reshape(C * C))
            kernel = taps[3 * row_tap + col_tap].reshape(C, C)
            back = jnp.einsum('oi,nohw->nihw', kernel, grad_z, precision=PRECISE)
            grad_pad = grad_pad.at[:, :, row_tap:row_tap + stride * height:stride, col_tap:col_tap + stride * width:stride].add(back)
    return (jnp.stack(tap_grads), grad_pad[:, :, 1:-1, 1:-1])

def reference(points, counts, cells, pfn_weight, pfn_gain, pfn_bias, conv_weight, bn_gain, bn_bias, cotangent):

    def hidden_of(args):
        return pillar_hidden(args[0][None], args[1][None], args[2][None], pfn_weight)

    def first_sums(args):
        hidden, is_valid = hidden_of(args)
        return (lax.optimization_barrier(jnp.sum(hidden * is_valid[:, None], axis=(0, 2, 3))), jnp.sum(is_valid))
    totals, counts_each = lax.map(first_sums, (points, counts, cells))
    count_all = jnp.sum(counts_each)
    mean_val = lax.optimization_barrier(jnp.sum(totals, axis=0)) / count_all

    def second_sums(args):
        hidden, is_valid = hidden_of(args)
        centred = hidden - channel_shape(mean_val, 4)
        return lax.optimization_barrier(jnp.sum(centred * centred * is_valid[:, None], axis=(0, 2, 3)))
    variance = lax.optimization_barrier(jnp.sum(lax.map(second_sums, (points, counts, cells)), axis=0)) / count_all
    inv_std = lax.rsqrt(variance + EPS)

    def to_grid(args):
        hidden, is_valid = hidden_of(args)
        pillar = normalize_pillars(hidden, is_valid, mean_val, inv_std, pfn_gain, pfn_bias)
        return scatter_pillars(pillar, args[2][None])[0]
    bev_grid = lax.map(to_grid, (points, counts, cells))
    activations = [bev_grid]
    normals = []
    for layer_idx in range(LAYERS):
        stride = 2 if layer_idx == 0 else 1
        weight = conv_weight[layer_idx]
        pre_norm = lax.map(lambda sweep: conv_forward(sweep[None], weight, stride)[0], activations[-1])
        mean_c = lax.optimization_barrier(jnp.mean(pre_norm, axis=(0, 2, 3)))
        centred = pre_norm - channel_shape(mean_c, 4)
        inv_c = lax.rsqrt(lax.optimization_barrier(jnp.mean(centred * centred, axis=(0, 2, 3))) + EPS)
        normed = centred * channel_shape(inv_c, 4)
        scaled = channel_shape(bn_gain[layer_idx], 4) * normed + channel_shape(bn_bias[layer_idx], 4)
        activations.append(jax.nn.silu(scaled))
        normals.append((normed, inv_c, scaled))
    upstream = cotangent
    grad_list = [None] * LAYERS
    gain_list = [None] * LAYERS
    bias_list = [None] * LAYERS
    pillar_grad = None
    for layer_idx in range(LAYERS - 1, -1, -1):
        stride = 2 if layer_idx == 0 else 1
        weight = conv_weight[layer_idx]
        normed, inv_c, scaled = normals[layer_idx]
        grad_y = upstream * silu_slope(scaled)
        sum_dy = lax.optimization_barrier(jnp.sum(grad_y, axis=(0, 2, 3)))
        sum_dyx = lax.optimization_barrier(jnp.sum(grad_y * normed, axis=(0, 2, 3)))
        entries = float(grad_y.shape[0] * grad_y.shape[2] * grad_y.shape[3])
        grad_z = channel_shape(bn_gain[layer_idx] * inv_c, 4) * (grad_y - channel_shape(sum_dy / entries, 4) - normed * channel_shape(sum_dyx / entries, 4))
        if layer_idx == 0:

            def back_first(args):
                grad_w, grad_in = conv_backward(args[0][None], weight, args[1][None], stride)
                plane = grad_in[0].reshape(grad_in.shape[1], GH * GW)
                return (grad_w, plane[:, args[2]])
            parts, pillar_grad = lax.map(back_first, (activations[0], grad_z, cells))
        else:

            def back_other(args):
                grad_w, grad_in = conv_backward(args[0][None], weight, args[1][None], stride)
                return (grad_w, grad_in[0])
            parts, upstream = lax.map(back_other, (activations[layer_idx], grad_z))
        grad_list[layer_idx] = lax.optimization_barrier(jnp.sum(parts, axis=0))
        gain_list[layer_idx] = sum_dyx
        bias_list[layer_idx] = sum_dy
    norm_grads = jnp.stack([jnp.stack(gain_list), jnp.stack(bias_list)])
    return (activations[-1], jnp.stack(grad_list), norm_grads, pillar_grad)
```

```python
import functools

import jax
import jax.numpy as jnp
from jax import lax
from jax.experimental import pallas as pl
from jax.experimental.pallas import tpu as pltpu
from jax.sharding import PartitionSpec as P

C = 64
MAXP = 32
LAYERS = 4
PILL = 256
COLS = 128
ROWS = 4
SW = 2
PLANE = ROWS * COLS
POS = SW * PLANE
K9 = 9 * C
EPS = 1e-05
CORES = 2
NZ = 8
NY = 4
LANES = 384
MESH = pl.DeviceIdType.MESH
F32 = jnp.float32
BF16 = jnp.bfloat16


def split(x):
    hi = x.astype(BF16)
    return hi, (x - hi.astype(F32)).astype(BF16)


def mm(a, b):
    return lax.dot_general(a, b, (((1,), (0,)), ((), ())), preferred_element_type=F32)


def mmt(a, b):
    return lax.dot_general(a, b, (((1,), (1,)), ((), ())), preferred_element_type=F32)


def fold(x):
    parts = [x[:, t * COLS : (t + 1) * COLS] for t in range(x.shape[1] // COLS)]
    while len(parts) > 1:
        parts = [parts[t] + parts[t + 1] for t in range(0, len(parts), 2)]
    return parts[0]


def wide(tile, n):
    return jnp.concatenate([tile] * n, axis=1)


def to_row(a, b):
    return jnp.sum(jnp.concatenate([a, b], axis=0).T, axis=0, keepdims=True)


def to_cols(row):
    full = jnp.broadcast_to(row, (2 * C, COLS)).T
    return full[:C], full[C:]


def col_shift(x, step):
    if step == 0:
        return x
    lane = lax.broadcasted_iota(jnp.int32, (x.shape[0], COLS), 1)
    edge = lane == (COLS - 1 if step > 0 else 0)
    turn = COLS - 1 if step > 0 else 1
    tiles = []
    for t in range(x.shape[1] // COLS):
        tile = pltpu.roll(x[:, t * COLS : (t + 1) * COLS], turn, 1)
        tiles.append(jnp.where(edge, 0.0, tile))
    return jnp.concatenate(tiles, axis=1)


def row_shift(x, step):
    if step == 0:
        return x
    none = jnp.zeros((x.shape[0], COLS), x.dtype)
    parts = []
    for s in range(x.shape[1] // PLANE):
        base = s * PLANE
        if step > 0:
            parts += [x[:, base + COLS : base + PLANE], none]
        else:
            parts += [none, x[:, base : base + PLANE - COLS]]
    return jnp.concatenate(parts, axis=1)


def store_taps(x, hi_ref, lo_ref, sign):
    for b in range(3):
        hi, lo = split(col_shift(x, sign * (b - 1)))
        for a in range(3):
            at = pl.ds((3 * a + b) * C, C)
            hi_ref[at, :] = row_shift(hi, sign * (a - 1))
            lo_ref[at, :] = row_shift(lo, sign * (a - 1))


def silu_parts(y):
    sg = 1.0 / (1.0 + jnp.exp(-y))
    return y * sg, sg * (1.0 + y * (1.0 - sg))


def step_kernel(
    size,
    points,
    counts,
    cells,
    pfn_w,
    pfn_g,
    pfn_b,
    w_fwd,
    w_bwd,
    bn_g,
    bn_b,
    cot,
    features,
    grads_out,
    norm_out,
    pillar_out,
    x9h,
    x9l,
    g9h,
    g9l,
    hot,
    xhat,
    slope,
    wf,
    wb,
    w0h,
    w0l,
    par,
    pwc,
    hmax,
    base,
    sq,
    u_ref,
    gy_ref,
    p_src,
    p_buf,
    s_src,
    s_buf,
    dw,
    rs_buf,
    x_src,
    x_buf,
    ag_src,
    full,
    p_send,
    p_recv,
    s_send,
    s_recv,
    g_send,
    g_recv,
):
    nx, ny, nz = size
    ga, gb = CORES * nz, nx * ny
    devices = ga * gb
    rack = lax.axis_index("rack")
    chip = lax.axis_index("chip")
    core = lax.rem(rack, CORES)
    my_x = rack // CORES
    my_z = lax.rem(chip, nz)
    my_y = chip // nz
    me = (core * nz + my_z, my_x * ny + my_y)
    groups = (ga, gb)

    def peer(phase, i):
        if phase == 0:
            return (my_x * CORES + i // nz, my_y * nz + lax.rem(i, nz))
        return ((i // ny) * CORES + core, lax.rem(i, ny) * nz + my_z)

    def each_peer(phase, act):
        def one(d, carry):
            act(lax.rem(me[phase] + d, groups[phase]))
            return carry

        lax.fori_loop(1, groups[phase], one, 0)

    barrier = pltpu.get_barrier_semaphore()
    for phase in range(2):
        each_peer(
            phase,
            lambda i, phase=phase: pl.semaphore_signal(
                barrier, inc=1, device_id=peer(phase, i), device_id_type=MESH
            ),
        )

    def spread(phase, src, buf, send, recv):
        def act(i):
            pltpu.make_async_remote_copy(
                src_ref=src,
                dst_ref=buf.at[me[phase]],
                send_sem=send,
                recv_sem=recv,
                device_id=peer(phase, i),
                device_id_type=MESH,
            ).start()

        each_peer(phase, act)

    def settle(phase, buf, sem):
        part = buf.at[pl.ds(0, groups[phase] - 1)]
        pltpu.make_async_copy(part, part, sem).wait()

    lane = lax.broadcasted_iota(jnp.int32, (1, COLS), 1)
    low = lane < C

    def columns(row_a, row_b):
        return to_cols(jnp.concatenate([row_a, row_b], axis=1))

    w = [pfn_w[f : f + 1, :] for f in range(9)]
    rows = [w[0] + w[4] + w[7], w[1] + w[5] + w[8], w[2] + w[6], w[3]] + w[4:9] + [w[8]]
    for k in range(0, 10, 2):
        pwc[k], pwc[k + 1] = columns(rows[k], rows[k + 1])

    half = lambda x, h: x[:, h * COLS : (h + 1) * COLS]
    slot = lax.broadcasted_iota(jnp.int32, (MAXP, PILL), 0)
    local_n = jnp.sum(counts[...].astype(F32))
    mean_tile = jnp.zeros((C, COLS), F32)
    for s in range(SW):
        n_row = counts[s : s + 1, :]
        n_f = n_row.astype(F32)
        ok = slot < n_row
        sums = [
            jnp.sum(jnp.where(ok, points[s, j], 0.0), axis=0, keepdims=True) for j in range(4)
        ]
        cell = cells[s : s + 1, :]
        col_pos = lax.rem(cell, 2 * COLS).astype(F32) * (1.0 / COLS) - 1.0
        row_pos = (cell // (2 * COLS)).astype(F32) * 0.25 - 1.0
        fixed = [sums[0] / n_f, sums[1] / n_f, sums[2] / n_f, col_pos, row_pos]
        for h in range(2):
            off = jnp.zeros((C, COLS), F32)
            for j in range(5):
                off = off - pwc[4 + j] * half(fixed[j], h)
            base[s, :, h * COLS : (h + 1) * COLS] = off
            acc = off * half(n_f, h)
            for j in range(4):
                acc = acc + pwc[j] * half(sums[j], h)
            mean_tile = mean_tile + acc
    local_mean = jnp.sum(mean_tile, axis=1, keepdims=True) / local_n

    pwc[9] = jnp.broadcast_to(local_mean, (C, COLS))
    for s in range(SW):
        base[s] = base[s] - wide(pwc[9], 2)

    grp = 16

    def channels(g, carry):
        at = pl.ds(pl.multiple_of(g * grp, grp), grp)
        wj = [pwc[j, at, :] for j in range(4)]

        def walk(k8, carry):
            tops, acc = list(carry[:-1]), carry[-1]
            first = pl.multiple_of(k8 * 8, 8)
            for s in range(SW):
                for h in range(2):
                    lanes = slice(h * COLS, (h + 1) * COLS)
                    off = base[s, at, lanes]
                    left = jnp.broadcast_to(counts[s : s + 1, lanes] - first, (grp, COLS))
                    pts = [points[s, j, pl.ds(first, 8), lanes] for j in range(4)]
                    for k in range(8):
                        value = off
                        for j in range(4):
                            value = value + wj[j] * pts[j][k : k + 1, :]
                        ok = left > k
                        top = jnp.where(ok, value, -3e38)
                        tops[2 * s + h] = jnp.maximum(tops[2 * s + h], top)
                        value = jnp.where(ok, value, 0.0)
                        acc = acc + value * value
            return (*tops, acc)

        start = [jnp.full((grp, COLS), -3e38, F32)] * (2 * SW)
        done = lax.fori_loop(0, MAXP // 8, walk, (*start, jnp.zeros((grp, COLS), F32)))
        for s in range(SW):
            for h in range(2):
                hmax[s, at, h * COLS : (h + 1) * COLS] = done[2 * s + h] + pwc[9, at, :]
        sq[at, :] = done[-1]
        return carry

    lax.fori_loop(0, C // grp, channels, 0)

    row = to_row(mean_tile, sq[...])
    row = jnp.where(low, row / local_n, row)
    payload = jnp.concatenate([row, jnp.full((1, COLS), local_n, F32)], axis=1)

    def merge_pfn(v):
        a, n = v[:, :, :COLS], v[:, :, COLS:]
        total = jnp.sum(n, axis=0)
        avg = jnp.sum(n * a, axis=0) / total
        dev = a - avg[None]
        spread_sq = jnp.sum(n * dev * dev, axis=0)
        both = jnp.where(low, avg, jnp.sum(a, axis=0) + pltpu.roll(spread_sq, C, 1))
        return jnp.concatenate([both, total], axis=1)

    pl.semaphore_wait(barrier, ga + gb - 2)
    p_src[0] = payload
    p_buf[0, me[0]] = payload
    spread(0, p_src.at[0], p_buf.at[0], p_send.at[0], p_recv.at[0])

    for s in range(SW):
        cell = cells[s : s + 1, :]
        r, c = cell // (2 * COLS), lax.rem(cell, 2 * COLS)
        spot = (
            (lax.rem(r, 2) * 2 + lax.rem(c, 2)) * PLANE + (r // 2) * COLS + c // 2
        )

        def fill(t, carry, s=s, spot=spot):
            ids = lax.broadcasted_iota(jnp.int32, (COLS, PILL), 0) + t * COLS
            hit = jnp.where(ids == spot, 1.0, 0.0)
            hot[s, pl.ds(pl.multiple_of(t * COLS, COLS), COLS), :] = hit.astype(BF16)
            return carry

        lax.fori_loop(0, 4 * PLANE // COLS, fill, 0)
    par[0], par[1] = columns(pfn_g[...], pfn_b[...])
    for l in range(LAYERS):
        par[2 + 2 * l], par[3 + 2 * l] = columns(bn_g[l : l + 1, :], bn_b[l : l + 1, :])

    def load_weights(l, carry):
        wf[l, :C, :], wf[l, C:, :] = split(w_fwd[l])
        wb[l, :C, :], wb[l, C:, :] = split(w_bwd[l])
        return carry

    lax.fori_loop(0, LAYERS, load_weights, 0)
    tap = lax.broadcasted_iota(jnp.int32, (C, K9), 1) // C
    parity = jnp.where(tap // 3 == 1, 0, 2) + jnp.where(lax.rem(tap, 3) == 1, 0, 1)
    for ph in range(4):
        hi, lo = split(jnp.where(parity == ph, w_bwd[0], 0.0))
        w0h[ph * C : (ph + 1) * C, :] = hi
        w0l[ph * C : (ph + 1) * C, :] = lo
    for l in range(LAYERS):
        dw[l, :, K9:] = jnp.zeros((C, 2 * LANES - K9), F32)

    settle(0, p_buf.at[0], p_recv.at[0])
    payload = merge_pfn(p_buf[0, pl.ds(0, ga)])
    p_src[1] = payload
    p_buf[1, me[1]] = payload
    spread(1, p_src.at[1], p_buf.at[1], p_send.at[1], p_recv.at[1])
    settle(1, p_buf.at[1], p_recv.at[1])
    payload = merge_pfn(p_buf[1, pl.ds(0, gb)])
    row, total = payload[:, :COLS], payload[:, COLS:]
    mean_c, inv_c = to_cols(jnp.where(low, row, lax.rsqrt(row / total + EPS)))
    scale = par[0] * inv_c

    for s in range(SW):
        pillar = jnp.concatenate(
            [
                jnp.maximum((half(hmax[s], h) - mean_c) * scale + par[1], 0.0)
                for h in range(2)
            ],
            axis=1,
        )
        hi, lo = split(pillar)
        both = jnp.concatenate([hi, lo], axis=0)
        lanes = slice(s * PLANE, (s + 1) * PLANE)
        for pr in range(2):
            for pc in range(2):
                ph = 2 * pr + pc
                plane = mmt(both, hot[s, ph * PLANE : (ph + 1) * PLANE, :])
                for b in (0, 2) if pc else (1,):
                    moved = col_shift(plane, -1 if b == 0 else 0).astype(BF16)
                    for a in (0, 2) if pr else (1,):
                        out = row_shift(moved, -1 if a == 0 else 0)
                        at = slice((3 * a + b) * C, (3 * a + b + 1) * C)
                        x9h[0, at, lanes] = out[:C]
                        x9l[0, at, lanes] = out[C:]

    def send_stat(rnd, phase, row):
        s_src[rnd, phase] = row
        s_buf[rnd, phase, me[phase]] = row
        spread(
            phase,
            s_src.at[rnd, phase],
            s_buf.at[rnd, phase],
            s_send.at[rnd, phase],
            s_recv.at[rnd, phase],
        )

    def take_stat(rnd, phase):
        settle(phase, s_buf.at[rnd, phase], s_recv.at[rnd, phase])
        return s_buf[rnd, phase, pl.ds(0, groups[phase])]

    def merge_norm(v, count):
        total = jnp.sum(v, axis=0)
        avg = total / v.shape[0]
        dev = v - avg[None]
        spread_sq = jnp.sum(dev * dev, axis=0) * count
        return jnp.where(low, avg, total + pltpu.roll(spread_sq, C, 1))

    def norm_layer(l, rnd):
        xh = x9h.at[l]
        xl = x9l.at[l]
        wide_z = mm(wf[l], xh[...])
        z = wide_z[:C] + wide_z[C:] + mm(wf[l, :C, :], xl[...])
        part = fold(z)
        m = jnp.sum(part, axis=1, keepdims=True) * (1.0 / POS)
        dev = z - m
        row = to_row(part, fold(dev * dev))
        send_stat(rnd, 0, jnp.where(low, row * (1.0 / POS), row))
        row = merge_norm(take_stat(rnd, 0), float(POS))
        send_stat(rnd, 1, row)
        row = merge_norm(take_stat(rnd, 1), float(POS * ga))
        mean_col, inv_col = to_cols(
            jnp.where(low, row, lax.rsqrt(row * (1.0 / (POS * devices)) + EPS))
        )
        normed = (z - wide(mean_col, POS // COLS)) * wide(inv_col, POS // COLS)
        gain, bias = par[2 + 2 * l], par[3 + 2 * l]
        y = wide(gain, POS // COLS) * normed + wide(bias, POS // COLS)
        act, slp = silu_parts(y)
        xhat[l] = normed
        slope[l] = slp
        par[10 + l] = gain * inv_col
        return act

    store_taps(norm_layer(0, 0), x9h.at[1], x9l.at[1], 1)

    def middle(l, carry):
        store_taps(norm_layer(l, l), x9h.at[l + 1], x9l.at[l + 1], 1)
        return carry

    lax.fori_loop(1, LAYERS - 1, middle, 0)
    act = norm_layer(LAYERS - 1, LAYERS - 1)
    for s in range(SW):
        for i in range(ROWS):
            at = s * PLANE + i * COLS
            features[s, :, i, :] = act[:, at : at + COLS]
            u_ref[:, at : at + COLS] = cot[s, :, i, :]

    def piece(ref, l, i):
        z_at = pl.multiple_of(lax.rem(i, nz) * (C // nz), C // nz)
        l_at = pl.multiple_of((i // nz) * LANES, COLS)
        return ref.at[l, pl.ds(z_at, C // nz), pl.ds(l_at, LANES)]

    def grad_start(l):
        gh = g9h[4 * C : 5 * C, :]
        both = jnp.concatenate([gh, g9l[4 * C : 5 * C, :]], axis=0)
        first = mmt(both, x9h[l])
        dw[l, :, :K9] = first[:C] + first[C:] + mmt(gh, x9l[l])

        def act(i):
            pltpu.make_async_remote_copy(
                src_ref=piece(dw, l, i),
                dst_ref=rs_buf.at[l, me[0]],
                send_sem=g_send.at[l, 0],
                recv_sem=g_recv.at[l, 0],
                device_id=peer(0, i),
                device_id_type=MESH,
            ).start()

        each_peer(0, act)
        rs_buf[l, me[0]] = piece(dw, l, me[0])[...]

    def grad_cross(l):
        settle(0, rs_buf.at[l], g_recv.at[l, 0])
        part = jnp.sum(rs_buf[l], axis=0)
        x_src[l] = part
        x_buf[l, me[1]] = part
        spread(1, x_src.at[l], x_buf.at[l], g_send.at[l, 1], g_recv.at[l, 1])

    def grad_back(l):
        settle(1, x_buf.at[l], g_recv.at[l, 1])
        part = jnp.sum(x_buf[l], axis=0)
        ag_src[l] = part

        def act(i):
            pltpu.make_async_remote_copy(
                src_ref=ag_src.at[l],
                dst_ref=piece(full, l, me[0]),
                send_sem=g_send.at[l, 2],
                recv_sem=g_recv.at[l, 2],
                device_id=peer(0, i),
                device_id_type=MESH,
            ).start()

        each_peer(0, act)
        piece(full, l, me[0])[...] = part

    total_m = 1.0 / (POS * devices)

    def sums_start(l, rnd):
        gy = u_ref[...] * slope[l]
        gy_ref[...] = gy
        send_stat(rnd, 0, to_row(fold(gy), fold(gy * xhat[l])))

    def sums_end(l, rnd):
        send_stat(rnd, 1, jnp.sum(take_stat(rnd, 0), axis=0))
        row = jnp.sum(take_stat(rnd, 1), axis=0)
        norm_out[1, pl.ds(l, 1), :] = row[:, :C]
        norm_out[0, pl.ds(l, 1), :] = pltpu.roll(row, C, 1)[:, :C]
        dy, dx = to_cols(row * total_m)
        n = POS // COLS
        return wide(par[10 + l], n) * (gy_ref[...] - wide(dy, n) - xhat[l] * wide(dx, n))

    def back(t, carry):
        l = LAYERS - 1 - t
        sums_start(l, LAYERS + t)

        @pl.when(t > 0)
        def _():
            grad_start(l + 1)

        @pl.when(t > 1)
        def _():
            grad_cross(l + 2)

        store_taps(sums_end(l, LAYERS + t), g9h, g9l, -1)
        first = mm(wb[l], g9h[...])
        u_ref[...] = first[:C] + first[C:] + mm(wb[l, :C, :], g9l[...])
        return carry

    lax.fori_loop(0, LAYERS - 1, back, 0)
    rnd = 2 * LAYERS - 1
    sums_start(0, rnd)
    grad_start(1)
    grad_cross(2)
    grad_back(3)
    gz = sums_end(0, rnd)
    for b in range(3):
        hi, lo = split(col_shift(gz, 1 if b == 0 else 0))
        for a in range(3):
            at = slice((3 * a + b) * C, (3 * a + b + 1) * C)
            g9h[at, :] = row_shift(hi, 1 if a == 0 else 0)
            g9l[at, :] = row_shift(lo, 1 if a == 0 else 0)
    grad_start(0)
    grad_cross(1)
    grad_back(2)
    u0 = mm(w0h[...], g9h[...]) + mm(w0l[...], g9h[...]) + mm(w0h[...], g9l[...])
    for s in range(SW):
        acc = jnp.zeros((2 * C, PILL), F32)
        for ph in range(4):
            hi, lo = split(u0[ph * C : (ph + 1) * C, s * PLANE : (s + 1) * PLANE])
            both = jnp.concatenate([hi, lo], axis=0)
            acc = acc + mm(both, hot[s, ph * PLANE : (ph + 1) * PLANE, :])
        pillar_out[s] = acc[:C] + acc[C:]
    grad_cross(0)
    grad_back(1)
    grad_back(0)

    for phase in range(2):
        settle(phase, p_buf.at[phase], p_send.at[phase])
        for r in range(2 * LAYERS):
            settle(phase, s_buf.at[r, phase], s_send.at[r, phase])
    for l in range(LAYERS):
        settle(0, rs_buf.at[l], g_send.at[l, 0])
        settle(1, x_buf.at[l], g_send.at[l, 1])
        settle(0, rs_buf.at[l], g_send.at[l, 2])
        settle(0, rs_buf.at[l], g_recv.at[l, 2])
        grads_out[l] = full[l, :, :K9]


def solution(mesh, ny=NY, nz=NZ):
    nx = mesh.shape["rack"] // CORES
    ga, gb = CORES * nz, nx * ny
    gmax = max(ga, gb)
    rows = C // nz

    def per_device(
        points, counts, cells, pfn_w, pfn_g, pfn_b, conv_w, bn_g, bn_b, cotangent
    ):
        taps = conv_w.reshape(LAYERS, 9, C, C)
        w_fwd = taps.transpose(0, 2, 1, 3).reshape(LAYERS, C, K9)
        w_bwd = taps.transpose(0, 3, 1, 2).reshape(LAYERS, C, K9)
        vmem = pl.BlockSpec(memory_space=pltpu.VMEM)
        dma = pltpu.SemaphoreType.DMA
        out = pl.pallas_call(
            functools.partial(step_kernel, (nx, ny, nz)),
            out_shape=(
                jax.ShapeDtypeStruct((SW, C, ROWS, COLS), F32),
                jax.ShapeDtypeStruct((LAYERS, C, K9), F32),
                jax.ShapeDtypeStruct((2, LAYERS, C), F32),
                jax.ShapeDtypeStruct((SW, C, PILL), F32),
            ),
            in_specs=[vmem] * 11,
            out_specs=(vmem,) * 4,
            scratch_shapes=[
                pltpu.VMEM((LAYERS, K9, POS), BF16),
                pltpu.VMEM((LAYERS, K9, POS), BF16),
                pltpu.VMEM((K9, POS), BF16),
                pltpu.VMEM((K9, POS), BF16),
                pltpu.VMEM((SW, 4 * PLANE, PILL), BF16),
                pltpu.VMEM((LAYERS, C, POS), F32),
                pltpu.VMEM((LAYERS, C, POS), F32),
                pltpu.VMEM((LAYERS, 2 * C, K9), BF16),
                pltpu.VMEM((LAYERS, 2 * C, K9), BF16),
                pltpu.VMEM((4 * C, K9), BF16),
                pltpu.VMEM((4 * C, K9), BF16),
                pltpu.VMEM((14, C, COLS), F32),
                pltpu.VMEM((10, C, COLS), F32),
                pltpu.VMEM((SW, C, PILL), F32),
                pltpu.VMEM((SW, C, PILL), F32),
                pltpu.VMEM((C, COLS), F32),
                pltpu.VMEM((C, POS), F32),
                pltpu.VMEM((C, POS), F32),
                pltpu.VMEM((2, 1, 2 * COLS), F32),
                pltpu.VMEM((2, gmax, 1, 2 * COLS), F32),
                pltpu.VMEM((2 * LAYERS, 2, 1, COLS), F32),
                pltpu.VMEM((2 * LAYERS, 2, gmax, 1, COLS), F32),
                pltpu.VMEM((LAYERS, C, 2 * LANES), F32),
                pltpu.VMEM((LAYERS, ga, rows, LANES), F32),
                pltpu.VMEM((LAYERS, rows, LANES), F32),
                pltpu.VMEM((LAYERS, gb, rows, LANES), F32),
                pltpu.VMEM((LAYERS, rows, LANES), F32),
                pltpu.VMEM((LAYERS, C, 2 * LANES), F32),
                dma((2,)),
                dma((2,)),
                dma((2 * LAYERS, 2)),
                dma((2 * LAYERS, 2)),
                dma((LAYERS, 3)),
                dma((LAYERS, 3)),
            ],
            compiler_params=pltpu.CompilerParams(
                collective_id=0, has_side_effects=True, vmem_limit_bytes=60 * 2**20
            ),
        )(
            points,
            counts,
            cells,
            pfn_w,
            pfn_g.reshape(1, C),
            pfn_b.reshape(1, C),
            w_fwd,
            w_bwd,
            bn_g,
            bn_b,
            cotangent,
        )
        features, grads, norm_grads, pillar_grad = out
        grads = grads.reshape(LAYERS, C, 9, C).transpose(0, 2, 1, 3).reshape(LAYERS, 9, C * C)
        return features, grads, norm_grads, pillar_grad

    split_all = ("rack", "chip")
    return jax.shard_map(
        per_device,
        mesh=mesh,
        in_specs=(
            P(split_all, None, None, None),
            P(split_all, None),
            P(split_all, None),
            P(),
            P(),
            P(),
            P(),
            P(),
            P(),
            P(split_all, None, None, None),
        ),
        out_specs=(
            P(split_all, None, None, None),
            P(),
            P(),
            P(split_all, None, None),
        ),
        check_vma=False,
    )
```

```python
import functools

import jax
import jax.numpy as jnp
from jax import lax
from jax.experimental import pallas as pl
from jax.experimental.pallas import tpu as pltpu
from jax.sharding import PartitionSpec as P

C = 64
MAXP = 32
LAYERS = 4
PILL = 256
COLS = 128
ROWS = 4
SW = 2
PLANE = ROWS * COLS
POS = SW * PLANE
K9 = 9 * C
EPS = 1e-05
CORES = 2
NZ = 8
NY = 4
LANES = 384
MESH = pl.DeviceIdType.MESH
F32 = jnp.float32
BF16 = jnp.bfloat16


def split(x):
    hi = x.astype(BF16)
    return hi, (x - hi.astype(F32)).astype(BF16)


def mm(a, b):
    return lax.dot_general(a, b, (((1,), (0,)), ((), ())), preferred_element_type=F32)


def mmt(a, b):
    return lax.dot_general(a, b, (((1,), (1,)), ((), ())), preferred_element_type=F32)


def fold(x):
    parts = [x[:, t * COLS : (t + 1) * COLS] for t in range(x.shape[1] // COLS)]
    while len(parts) > 1:
        parts = [parts[t] + parts[t + 1] for t in range(0, len(parts), 2)]
    return parts[0]


def wide(tile, n):
    return jnp.concatenate([tile] * n, axis=1)


def to_row(a, b):
    return jnp.sum(jnp.concatenate([a, b], axis=0).T, axis=0, keepdims=True)


def to_cols(row):
    full = jnp.broadcast_to(row, (2 * C, COLS)).T
    return full[:C], full[C:]


def col_shift(x, step):
    if step == 0:
        return x
    lane = lax.broadcasted_iota(jnp.int32, (x.shape[0], COLS), 1)
    edge = lane == (COLS - 1 if step > 0 else 0)
    turn = COLS - 1 if step > 0 else 1
    tiles = []
    for t in range(x.shape[1] // COLS):
        tile = pltpu.roll(x[:, t * COLS : (t + 1) * COLS], turn, 1)
        tiles.append(jnp.where(edge, 0.0, tile))
    return jnp.concatenate(tiles, axis=1)


def row_shift(x, step):
    if step == 0:
        return x
    none = jnp.zeros((x.shape[0], COLS), x.dtype)
    parts = []
    for s in range(x.shape[1] // PLANE):
        base = s * PLANE
        if step > 0:
            parts += [x[:, base + COLS : base + PLANE], none]
        else:
            parts += [none, x[:, base : base + PLANE - COLS]]
    return jnp.concatenate(parts, axis=1)


def store_taps(x, hi_ref, lo_ref, sign):
    for b in range(3):
        hi, lo = split(col_shift(x, sign * (b - 1)))
        for a in range(3):
            at = pl.ds((3 * a + b) * C, C)
            hi_ref[at, :] = row_shift(hi, sign * (a - 1))
            lo_ref[at, :] = row_shift(lo, sign * (a - 1))


def silu_parts(y):
    sg = 1.0 / (1.0 + jnp.exp(-y))
    return y * sg, sg * (1.0 + y * (1.0 - sg))


def step_kernel(
    size,
    points,
    counts,
    cells,
    pfn_w,
    pfn_g,
    pfn_b,
    w_fwd,
    w_bwd,
    bn_g,
    bn_b,
    cot,
    features,
    grads_out,
    norm_out,
    pillar_out,
    x9h,
    x9l,
    g9h,
    g9l,
    hot,
    xhat,
    slope,
    wf,
    wb,
    w0h,
    w0l,
    par,
    pwc,
    hmax,
    base,
    sq,
    u_ref,
    gy_ref,
    p_src,
    p_buf,
    s_src,
    s_buf,
    dw,
    rs_buf,
    x_src,
    x_buf,
    ag_src,
    full,
    c_src,
    c_buf,
    cx_src,
    cx_buf,
    trio,
    c_send,
    c_recv,
    p_send,
    p_recv,
    s_send,
    s_recv,
    g_send,
    g_recv,
):
    nx, ny, nz = size
    ga, gb = CORES * nx * ny, nz
    devices = ga * gb
    rack = lax.axis_index("rack")
    chip = lax.axis_index("chip")
    core = lax.rem(rack, CORES)
    my_x = rack // CORES
    my_z = lax.rem(chip, nz)
    my_y = chip // nz
    mine = my_x * ny + my_y
    me = (core * (nx * ny) + mine, my_z)
    groups = (ga, gb)

    def peer(phase, i):
        if phase == 0:
            at = lax.rem(i, nx * ny)
            return ((at // ny) * CORES + i // (nx * ny), lax.rem(at, ny) * nz + my_z)
        return (rack, my_y * nz + i)

    def each_peer(phase, act, unroll=False):
        if unroll:
            for d in range(1, groups[phase]):
                act(lax.rem(me[phase] + d, groups[phase]))
            return

        def one(d, carry):
            act(lax.rem(me[phase] + d, groups[phase]))
            return carry

        lax.fori_loop(1, groups[phase], one, 0)

    barrier = pltpu.get_barrier_semaphore()
    for phase in range(2):
        each_peer(
            phase,
            lambda i, phase=phase: pl.semaphore_signal(
                barrier, inc=1, device_id=peer(phase, i), device_id_type=MESH
            ),
        )

    def spread(phase, src, buf, send, recv, unroll=False):
        def act(i):
            pltpu.make_async_remote_copy(
                src_ref=src,
                dst_ref=buf.at[me[phase]],
                send_sem=send,
                recv_sem=recv,
                device_id=peer(phase, i),
                device_id_type=MESH,
            ).start()

        each_peer(phase, act, unroll)

    def settle(phase, buf, sem):
        part = buf.at[pl.ds(0, groups[phase] - 1)]
        pltpu.make_async_copy(part, part, sem).wait()

    lane = lax.broadcasted_iota(jnp.int32, (1, COLS), 1)
    low = lane < C

    def columns(row_a, row_b):
        return to_cols(jnp.concatenate([row_a, row_b], axis=1))

    w = [pfn_w[f : f + 1, :] for f in range(9)]
    rows = [w[0] + w[4] + w[7], w[1] + w[5] + w[8], w[2] + w[6], w[3]] + w[4:9] + [w[8]]
    for k in range(0, 10, 2):
        pwc[k], pwc[k + 1] = columns(rows[k], rows[k + 1])

    half = lambda x, h: x[:, h * COLS : (h + 1) * COLS]
    slot = lax.broadcasted_iota(jnp.int32, (MAXP, PILL), 0)
    local_n = jnp.sum(counts[...].astype(F32))
    mean_tile = jnp.zeros((C, COLS), F32)
    for s in range(SW):
        n_row = counts[s : s + 1, :]
        n_f = n_row.astype(F32)
        ok = slot < n_row
        sums = [
            jnp.sum(jnp.where(ok, points[s, j], 0.0), axis=0, keepdims=True) for j in range(4)
        ]
        cell = cells[s : s + 1, :]
        col_pos = lax.rem(cell, 2 * COLS).astype(F32) * (1.0 / COLS) - 1.0
        row_pos = (cell // (2 * COLS)).astype(F32) * 0.25 - 1.0
        fixed = [sums[0] / n_f, sums[1] / n_f, sums[2] / n_f, col_pos, row_pos]
        for h in range(2):
            off = jnp.zeros((C, COLS), F32)
            for j in range(5):
                off = off - pwc[4 + j] * half(fixed[j], h)
            base[s, :, h * COLS : (h + 1) * COLS] = off
            acc = off * half(n_f, h)
            for j in range(4):
                acc = acc + pwc[j] * half(sums[j], h)
            mean_tile = mean_tile + acc
    local_mean = jnp.sum(mean_tile, axis=1, keepdims=True) / local_n

    pwc[9] = jnp.broadcast_to(local_mean, (C, COLS))
    for s in range(SW):
        base[s] = base[s] - wide(pwc[9], 2)

    grp = 16

    def channels(g, carry):
        at = pl.ds(pl.multiple_of(g * grp, grp), grp)
        wj = [pwc[j, at, :] for j in range(4)]

        def walk(k8, carry):
            tops, acc = list(carry[:-1]), carry[-1]
            first = pl.multiple_of(k8 * 8, 8)
            for s in range(SW):
                for h in range(2):
                    lanes = slice(h * COLS, (h + 1) * COLS)
                    off = base[s, at, lanes]
                    left = jnp.broadcast_to(counts[s : s + 1, lanes] - first, (grp, COLS))
                    pts = [points[s, j, pl.ds(first, 8), lanes] for j in range(4)]
                    for k in range(8):
                        value = off
                        for j in range(4):
                            value = value + wj[j] * pts[j][k : k + 1, :]
                        ok = left > k
                        top = jnp.where(ok, value, -3e38)
                        tops[2 * s + h] = jnp.maximum(tops[2 * s + h], top)
                        value = jnp.where(ok, value, 0.0)
                        acc = acc + value * value
            return (*tops, acc)

        start = [jnp.full((grp, COLS), -3e38, F32)] * (2 * SW)
        done = lax.fori_loop(0, MAXP // 8, walk, (*start, jnp.zeros((grp, COLS), F32)))
        for s in range(SW):
            for h in range(2):
                hmax[s, at, h * COLS : (h + 1) * COLS] = done[2 * s + h] + pwc[9, at, :]
        sq[at, :] = done[-1]
        return carry

    lax.fori_loop(0, C // grp, channels, 0)

    row = to_row(mean_tile, sq[...])
    row = jnp.where(low, row / local_n, row)
    payload = jnp.concatenate([row, jnp.full((1, COLS), local_n, F32)], axis=1)

    def merge_pfn(v):
        a, n = v[:, :, :COLS], v[:, :, COLS:]
        total = jnp.sum(n, axis=0)
        avg = jnp.sum(n * a, axis=0) / total
        dev = a - avg[None]
        spread_sq = jnp.sum(n * dev * dev, axis=0)
        both = jnp.where(low, avg, jnp.sum(a, axis=0) + pltpu.roll(spread_sq, C, 1))
        return jnp.concatenate([both, total], axis=1)

    pl.semaphore_wait(barrier, ga + gb - 2)
    p_src[0] = payload
    p_buf[0, me[0]] = payload
    spread(0, p_src.at[0], p_buf.at[0], p_send.at[0], p_recv.at[0], True)

    for s in range(SW):
        cell = cells[s : s + 1, :]
        r, c = cell // (2 * COLS), lax.rem(cell, 2 * COLS)
        spot = (
            (lax.rem(r, 2) * 2 + lax.rem(c, 2)) * PLANE + (r // 2) * COLS + c // 2
        )

        def fill(t, carry, s=s, spot=spot):
            ids = lax.broadcasted_iota(jnp.int32, (COLS, PILL), 0) + t * COLS
            hit = jnp.where(ids == spot, 1.0, 0.0)
            hot[s, pl.ds(pl.multiple_of(t * COLS, COLS), COLS), :] = hit.astype(BF16)
            return carry

        lax.fori_loop(0, 4 * PLANE // COLS, fill, 0)
    par[0], par[1] = columns(pfn_g[...], pfn_b[...])
    for l in range(LAYERS):
        par[2 + 2 * l], par[3 + 2 * l] = columns(bn_g[l : l + 1, :], bn_b[l : l + 1, :])

    def load_weights(l, carry):
        wf[l, :C, :], wf[l, C:, :] = split(w_fwd[l])
        wb[l, :C, :], wb[l, C:, :] = split(w_bwd[l])
        return carry

    lax.fori_loop(0, LAYERS, load_weights, 0)
    tap = lax.broadcasted_iota(jnp.int32, (C, K9), 1) // C
    parity = jnp.where(tap // 3 == 1, 0, 2) + jnp.where(lax.rem(tap, 3) == 1, 0, 1)
    for ph in range(4):
        hi, lo = split(jnp.where(parity == ph, w_bwd[0], 0.0))
        w0h[ph * C : (ph + 1) * C, :] = hi
        w0l[ph * C : (ph + 1) * C, :] = lo

    settle(0, p_buf.at[0], p_recv.at[0])
    payload = merge_pfn(p_buf[0, pl.ds(0, ga)])
    p_src[1] = payload
    p_buf[1, me[1]] = payload
    spread(1, p_src.at[1], p_buf.at[1], p_send.at[1], p_recv.at[1], True)
    settle(1, p_buf.at[1], p_recv.at[1])
    payload = merge_pfn(p_buf[1, pl.ds(0, gb)])
    row, total = payload[:, :COLS], payload[:, COLS:]
    mean_c, inv_c = to_cols(jnp.where(low, row, lax.rsqrt(row / total + EPS)))
    scale = par[0] * inv_c

    for s in range(SW):
        pillar = jnp.concatenate(
            [
                jnp.maximum((half(hmax[s], h) - mean_c) * scale + par[1], 0.0)
                for h in range(2)
            ],
            axis=1,
        )
        hi, lo = split(pillar)
        both = jnp.concatenate([hi, lo], axis=0)
        lanes = slice(s * PLANE, (s + 1) * PLANE)
        for pr in range(2):
            for pc in range(2):
                ph = 2 * pr + pc
                plane = mmt(both, hot[s, ph * PLANE : (ph + 1) * PLANE, :])
                for b in (0, 2) if pc else (1,):
                    moved = col_shift(plane, -1 if b == 0 else 0).astype(BF16)
                    for a in (0, 2) if pr else (1,):
                        out = row_shift(moved, -1 if a == 0 else 0)
                        at = slice((3 * a + b) * C, (3 * a + b + 1) * C)
                        x9h[0, at, lanes] = out[:C]
                        x9l[0, at, lanes] = out[C:]

    def send_stat(rnd, phase, row):
        s_src[rnd, phase] = row
        s_buf[rnd, phase, me[phase]] = row
        spread(
            phase,
            s_src.at[rnd, phase],
            s_buf.at[rnd, phase],
            s_send.at[rnd, phase],
            s_recv.at[rnd, phase],
            True,
        )

    def take_stat(rnd, phase):
        settle(phase, s_buf.at[rnd, phase], s_recv.at[rnd, phase])
        return s_buf[rnd, phase, pl.ds(0, groups[phase])]

    def merge_norm(v, count):
        total = jnp.sum(v, axis=0)
        avg = total / v.shape[0]
        dev = v - avg[None]
        spread_sq = jnp.sum(dev * dev, axis=0) * count
        return jnp.where(low, avg, total + pltpu.roll(spread_sq, C, 1))

    def norm_layer(l, rnd, meanwhile=None):
        xh = x9h.at[l]
        xl = x9l.at[l]
        wide_z = mm(wf[l], xh[...])
        z = wide_z[:C] + wide_z[C:] + mm(wf[l, :C, :], xl[...])
        part = fold(z)
        m = jnp.sum(part, axis=1, keepdims=True) * (1.0 / POS)
        dev = z - m
        row = to_row(part, fold(dev * dev))
        send_stat(rnd, 0, jnp.where(low, row * (1.0 / POS), row))
        if meanwhile is not None:
            meanwhile()
        row = merge_norm(take_stat(rnd, 0), float(POS))
        send_stat(rnd, 1, row)
        row = merge_norm(take_stat(rnd, 1), float(POS * ga))
        mean_col, inv_col = to_cols(
            jnp.where(low, row, lax.rsqrt(row * (1.0 / (POS * devices)) + EPS))
        )
        normed = (z - wide(mean_col, POS // COLS)) * wide(inv_col, POS // COLS)
        gain, bias = par[2 + 2 * l], par[3 + 2 * l]
        y = wide(gain, POS // COLS) * normed + wide(bias, POS // COLS)
        act, slp = silu_parts(y)
        xhat[l] = normed
        slope[l] = slp
        par[10 + l] = gain * inv_col
        return act

    rows = C // (nx * ny)
    pad = jnp.zeros((C, 2 * LANES - K9), F32)

    def pieces(value):
        value = jnp.concatenate([value, pad], axis=1)
        for i in range(ga):
            r_at = (i % (nx * ny)) * rows
            l_at = (i // (nx * ny)) * LANES
            yield i, value[r_at : r_at + rows, l_at : l_at + LANES]

    def scatter(src, buf, send, recv):
        def act(i):
            pltpu.make_async_remote_copy(
                src_ref=src.at[i],
                dst_ref=buf.at[me[0]],
                send_sem=send,
                recv_sem=recv,
                device_id=peer(0, i),
                device_id_type=MESH,
            ).start()

        each_peer(0, act)
        buf[me[0]] = src[me[0]]

    def fixed_start():
        hi, lo = split(xhat[0])
        ones = jnp.ones((C, POS), BF16)
        first = mmt(jnp.concatenate([hi, lo, ones], axis=0), x9h[0])
        second = mmt(jnp.concatenate([hi, ones], axis=0), x9l[0])
        corr = first[:C] + first[C : 2 * C] + second[:C]
        plain = first[2 * C : 3 * C] + second[C : 2 * C]
        for i, part in pieces(corr):
            c_src[i, :rows, :] = part
        for i, part in pieces(plain):
            c_src[i, rows:, :] = part
        scatter(c_src, c_buf, c_send.at[0], c_recv.at[0])

    def fixed_cross():
        settle(0, c_buf, c_recv.at[0])
        part = jnp.sum(c_buf[...], axis=0)
        cx_src[...] = part
        cx_buf[me[1]] = part
        spread(1, cx_src, cx_buf, c_send.at[1], c_recv.at[1])

    store_taps(norm_layer(0, 0), x9h.at[1], x9l.at[1], 1)

    def middle(l, carry):
        def meanwhile():
            pl.when(l == 1)(fixed_start)
            pl.when(l == 2)(fixed_cross)

        store_taps(norm_layer(l, l, meanwhile), x9h.at[l + 1], x9l.at[l + 1], 1)
        return carry

    lax.fori_loop(1, LAYERS - 1, middle, 0)
    act = norm_layer(LAYERS - 1, LAYERS - 1)
    for s in range(SW):
        for i in range(ROWS):
            at = s * PLANE + i * COLS
            features[s, :, i, :] = act[:, at : at + COLS]
            u_ref[:, at : at + COLS] = cot[s, :, i, :]

    def grad_start(l, gh=None, gl=None):
        if gh is None:
            gh, gl = g9h[4 * C : 5 * C, :], g9l[4 * C : 5 * C, :]
        both = jnp.concatenate([gh, gl], axis=0)
        first = mmt(both, x9h[l])
        for i, part in pieces(first[:C] + first[C:] + mmt(gh, x9l[l])):
            dw[l, i] = part
        scatter(dw.at[l], rs_buf.at[l], g_send.at[l, 0], g_recv.at[l, 0])

    def grad_cross(l):
        settle(0, rs_buf.at[l], g_recv.at[l, 0])
        part = jnp.sum(rs_buf[l], axis=0)
        x_src[l] = part
        x_buf[l, me[1]] = part
        spread(1, x_src.at[l], x_buf.at[l], g_send.at[l, 1], g_recv.at[l, 1])

    def grad_back(l, finish=None):
        settle(1, x_buf.at[l], g_recv.at[l, 1])
        part = jnp.sum(x_buf[l], axis=0)
        if finish is not None:
            part = finish(part)
        ag_src[l] = part

        spread(0, ag_src.at[l], full.at[l], g_send.at[l, 2], g_recv.at[l, 2])
        full[l, me[0]] = part

    total_m = 1.0 / (POS * devices)

    def sums_start(l, rnd):
        gy = u_ref[...] * slope[l]
        gy_ref[...] = gy
        send_stat(rnd, 0, to_row(fold(gy), fold(gy * xhat[l])))

    def sums_cross(rnd):
        send_stat(rnd, 1, jnp.sum(take_stat(rnd, 0), axis=0))

    def sums_end(l, rnd):
        row = jnp.sum(take_stat(rnd, 1), axis=0)
        norm_out[1, pl.ds(l, 1), :] = row[:, :C]
        norm_out[0, pl.ds(l, 1), :] = pltpu.roll(row, C, 1)[:, :C]
        return to_cols(row * total_m)

    def grad_z(l, dy, dx):
        n = POS // COLS
        return wide(par[10 + l], n) * (gy_ref[...] - wide(dy, n) - xhat[l] * wide(dx, n))

    def back(t, carry):
        l = LAYERS - 1 - t
        sums_start(l, LAYERS + t)

        @pl.when(t > 0)
        def _():
            grad_start(l + 1)

        @pl.when(t > 1)
        def _():
            grad_back(l + 2)

        sums_cross(LAYERS + t)

        @pl.when(t > 0)
        def _():
            grad_cross(l + 1)

        store_taps(grad_z(l, *sums_end(l, LAYERS + t)), g9h, g9l, -1)
        first = mm(wb[l], g9h[...])
        u_ref[...] = first[:C] + first[C:] + mm(wb[l, :C, :], g9l[...])
        return carry

    lax.fori_loop(0, LAYERS - 1, back, 0)
    rnd = 2 * LAYERS - 1
    sums_start(0, rnd)
    grad_start(0, *split(gy_ref[...]))
    grad_start(1)
    grad_back(2)
    sums_cross(rnd)
    grad_cross(0)
    grad_cross(1)
    settle(1, cx_buf, c_recv.at[1])
    fixed = jnp.sum(cx_buf[...], axis=0)
    dy, dx = sums_end(0, rnd)
    for k, tile in enumerate((dy, dx, par[10])):
        for q in range(nx * ny):
            trio[k, q] = tile[q * rows : (q + 1) * rows]

    def finish(part):
        dy_m, dx_m, k_m = [wide(trio[k, mine], LANES // COLS) for k in range(3)]
        return k_m * (part - fixed[rows:] * dy_m - fixed[:rows] * dx_m)

    grad_back(0, finish)
    grad_back(1)
    gz = grad_z(0, dy, dx)
    for b in range(3):
        hi, lo = split(col_shift(gz, 1 if b == 0 else 0))
        for a in range(3):
            at = slice((3 * a + b) * C, (3 * a + b + 1) * C)
            g9h[at, :] = row_shift(hi, 1 if a == 0 else 0)
            g9l[at, :] = row_shift(lo, 1 if a == 0 else 0)
    u0 = mm(w0h[...], g9h[...]) + mm(w0l[...], g9h[...]) + mm(w0h[...], g9l[...])
    for s in range(SW):
        acc = jnp.zeros((2 * C, PILL), F32)
        for ph in range(4):
            hi, lo = split(u0[ph * C : (ph + 1) * C, s * PLANE : (s + 1) * PLANE])
            both = jnp.concatenate([hi, lo], axis=0)
            acc = acc + mm(both, hot[s, ph * PLANE : (ph + 1) * PLANE, :])
        pillar_out[s] = acc[:C] + acc[C:]

    for phase in range(2):
        settle(phase, p_buf.at[phase], p_send.at[phase])
        for r in range(2 * LAYERS):
            settle(phase, s_buf.at[r, phase], s_send.at[r, phase])
    settle(0, c_buf, c_send.at[0])
    settle(1, cx_buf, c_send.at[1])
    for l in range(LAYERS):
        settle(0, rs_buf.at[l], g_send.at[l, 0])
        settle(1, x_buf.at[l], g_send.at[l, 1])
        settle(0, rs_buf.at[l], g_send.at[l, 2])
        settle(0, rs_buf.at[l], g_recv.at[l, 2])
        for i in range(ga):
            r_at = (i % (nx * ny)) * rows
            l_at = (i // (nx * ny)) * LANES
            width = min(LANES, K9 - l_at)
            grads_out[l, r_at : r_at + rows, l_at : l_at + width] = full[l, i, :, :width]


def solution(mesh, ny=NY, nz=NZ):
    nx = mesh.shape["rack"] // CORES
    ga, gb = CORES * nx * ny, nz
    gmax = max(ga, gb)
    rows = C // (nx * ny)

    def per_device(
        points, counts, cells, pfn_w, pfn_g, pfn_b, conv_w, bn_g, bn_b, cotangent
    ):
        taps = conv_w.reshape(LAYERS, 9, C, C)
        w_fwd = taps.transpose(0, 2, 1, 3).reshape(LAYERS, C, K9)
        w_bwd = taps.transpose(0, 3, 1, 2).reshape(LAYERS, C, K9)
        vmem = pl.BlockSpec(memory_space=pltpu.VMEM)
        dma = pltpu.SemaphoreType.DMA
        out = pl.pallas_call(
            functools.partial(step_kernel, (nx, ny, nz)),
            out_shape=(
                jax.ShapeDtypeStruct((SW, C, ROWS, COLS), F32),
                jax.ShapeDtypeStruct((LAYERS, C, K9), F32),
                jax.ShapeDtypeStruct((2, LAYERS, C), F32),
                jax.ShapeDtypeStruct((SW, C, PILL), F32),
            ),
            in_specs=[vmem] * 11,
            out_specs=(vmem,) * 4,
            scratch_shapes=[
                pltpu.VMEM((LAYERS, K9, POS), BF16),
                pltpu.VMEM((LAYERS, K9, POS), BF16),
                pltpu.VMEM((K9, POS), BF16),
                pltpu.VMEM((K9, POS), BF16),
                pltpu.VMEM((SW, 4 * PLANE, PILL), BF16),
                pltpu.VMEM((LAYERS, C, POS), F32),
                pltpu.VMEM((LAYERS, C, POS), F32),
                pltpu.VMEM((LAYERS, 2 * C, K9), BF16),
                pltpu.VMEM((LAYERS, 2 * C, K9), BF16),
                pltpu.VMEM((4 * C, K9), BF16),
                pltpu.VMEM((4 * C, K9), BF16),
                pltpu.VMEM((14, C, COLS), F32),
                pltpu.VMEM((10, C, COLS), F32),
                pltpu.VMEM((SW, C, PILL), F32),
                pltpu.VMEM((SW, C, PILL), F32),
                pltpu.VMEM((C, COLS), F32),
                pltpu.VMEM((C, POS), F32),
                pltpu.VMEM((C, POS), F32),
                pltpu.VMEM((2, 1, 2 * COLS), F32),
                pltpu.VMEM((2, gmax, 1, 2 * COLS), F32),
                pltpu.VMEM((2 * LAYERS, 2, 1, COLS), F32),
                pltpu.VMEM((2 * LAYERS, 2, gmax, 1, COLS), F32),
                pltpu.VMEM((LAYERS, ga, rows, LANES), F32),
                pltpu.VMEM((LAYERS, ga, rows, LANES), F32),
                pltpu.VMEM((LAYERS, rows, LANES), F32),
                pltpu.VMEM((LAYERS, gb, rows, LANES), F32),
                pltpu.VMEM((LAYERS, rows, LANES), F32),
                pltpu.VMEM((LAYERS, ga, rows, LANES), F32),
                pltpu.VMEM((ga, 2 * rows, LANES), F32),
                pltpu.VMEM((ga, 2 * rows, LANES), F32),
                pltpu.VMEM((2 * rows, LANES), F32),
                pltpu.VMEM((gb, 2 * rows, LANES), F32),
                pltpu.VMEM((3, ga // CORES, rows, COLS), F32),
                dma((2,)),
                dma((2,)),
                dma((2,)),
                dma((2,)),
                dma((2 * LAYERS, 2)),
                dma((2 * LAYERS, 2)),
                dma((LAYERS, 3)),
                dma((LAYERS, 3)),
            ],
            compiler_params=pltpu.CompilerParams(
                collective_id=0, has_side_effects=True, vmem_limit_bytes=60 * 2**20
            ),
        )(
            points,
            counts,
            cells,
            pfn_w,
            pfn_g.reshape(1, C),
            pfn_b.reshape(1, C),
            w_fwd,
            w_bwd,
            bn_g,
            bn_b,
            cotangent,
        )
        features, grads, norm_grads, pillar_grad = out
        grads = grads.reshape(LAYERS, C, 9, C).transpose(0, 2, 1, 3).reshape(LAYERS, 9, C * C)
        return features, grads, norm_grads, pillar_grad

    split_all = ("rack", "chip")
    return jax.shard_map(
        per_device,
        mesh=mesh,
        in_specs=(
            P(split_all, None, None, None),
            P(split_all, None),
            P(split_all, None),
            P(),
            P(),
            P(),
            P(),
            P(),
            P(),
            P(split_all, None, None, None),
        ),
        out_specs=(
            P(split_all, None, None, None),
            P(),
            P(),
            P(split_all, None, None),
        ),
        check_vma=False,
    )
```

```python
import functools

import jax
import jax.numpy as jnp
from jax import lax
from jax.experimental import pallas as pl
from jax.experimental.pallas import tpu as pltpu
from jax.sharding import PartitionSpec as P

C = 64
MAXP = 32
LAYERS = 4
PILL = 256
COLS = 128
ROWS = 4
SW = 2
PLANE = ROWS * COLS
POS = SW * PLANE
K9 = 9 * C
EPS = 1e-05
CORES = 2
NZ = 8
NY = 4
LANES = 384
VLIM = 60
MESH = pl.DeviceIdType.MESH
F32 = jnp.float32
BF16 = jnp.bfloat16


def split(x):
    hi = x.astype(BF16)
    return hi, (x - hi.astype(F32)).astype(BF16)


def mm(a, b):
    return lax.dot_general(a, b, (((1,), (0,)), ((), ())), preferred_element_type=F32)


def mmt(a, b):
    return lax.dot_general(a, b, (((1,), (1,)), ((), ())), preferred_element_type=F32)


def fold(x):
    parts = [x[:, t * COLS : (t + 1) * COLS] for t in range(x.shape[1] // COLS)]
    while len(parts) > 1:
        parts = [parts[t] + parts[t + 1] for t in range(0, len(parts), 2)]
    return parts[0]


def wide(tile, n):
    return jnp.concatenate([tile] * n, axis=1)


def to_row(a, b):
    return jnp.sum(jnp.concatenate([a, b], axis=0).T, axis=0, keepdims=True)


def to_cols(row):
    full = jnp.broadcast_to(row, (2 * C, COLS)).T
    return full[:C], full[C:]


def col_shift(x, step):
    if step == 0:
        return x
    lane = lax.broadcasted_iota(jnp.int32, (x.shape[0], COLS), 1)
    edge = lane == (COLS - 1 if step > 0 else 0)
    turn = COLS - 1 if step > 0 else 1
    tiles = []
    for t in range(x.shape[1] // COLS):
        tile = pltpu.roll(x[:, t * COLS : (t + 1) * COLS], turn, 1)
        tiles.append(jnp.where(edge, 0.0, tile))
    return jnp.concatenate(tiles, axis=1)


def row_shift(x, step):
    if step == 0:
        return x
    none = jnp.zeros((x.shape[0], COLS), x.dtype)
    parts = []
    for s in range(x.shape[1] // PLANE):
        base = s * PLANE
        if step > 0:
            parts += [x[:, base + COLS : base + PLANE], none]
        else:
            parts += [none, x[:, base : base + PLANE - COLS]]
    return jnp.concatenate(parts, axis=1)


def store_taps(x, hi_ref, lo_ref, sign):
    for b in range(3):
        hi, lo = split(col_shift(x, sign * (b - 1)))
        for a in range(3):
            at = pl.ds((3 * a + b) * C, C)
            hi_ref[at, :] = row_shift(hi, sign * (a - 1))
            lo_ref[at, :] = row_shift(lo, sign * (a - 1))


def silu_parts(y):
    sg = 1.0 / (1.0 + jnp.exp(-y))
    return y * sg, sg * (1.0 + y * (1.0 - sg))


def step_kernel(
    size,
    points,
    counts,
    cells,
    pfn_w,
    pfn_g,
    pfn_b,
    conv_w,
    bn_g,
    bn_b,
    cot,
    features,
    grads_out,
    norm_out,
    pillar_out,
    x9h,
    x9l,
    g9h,
    g9l,
    hot,
    xhat,
    slope,
    wf,
    wb,
    w0h,
    w0l,
    w_raw,
    par,
    pwc,
    hmax,
    base,
    sq,
    u_ref,
    gy_ref,
    p_src,
    p_buf,
    s_src,
    s_buf,
    dw,
    rs_buf,
    x_src,
    x_buf,
    ag_src,
    full,
    c_src,
    c_buf,
    cx_src,
    cx_buf,
    trio,
    c_send,
    c_recv,
    p_send,
    p_recv,
    s_send,
    s_recv,
    g_send,
    g_recv,
):
    nx, ny, nz = size
    ga, gb = CORES * nx * ny, nz
    devices = ga * gb
    rack = lax.axis_index("rack")
    chip = lax.axis_index("chip")
    core = lax.rem(rack, CORES)
    my_x = rack // CORES
    my_z = lax.rem(chip, nz)
    my_y = chip // nz
    mine = my_x * ny + my_y
    me = (core * (nx * ny) + mine, my_z)
    groups = (ga, gb)

    def peer(phase, i):
        if phase == 0:
            at = lax.rem(i, nx * ny)
            return ((at // ny) * CORES + i // (nx * ny), lax.rem(at, ny) * nz + my_z)
        return (rack, my_y * nz + i)

    def each_peer(phase, act, unroll=False):
        if unroll:
            for d in range(1, groups[phase]):
                act(lax.rem(me[phase] + d, groups[phase]))
            return

        def one(d, carry):
            act(lax.rem(me[phase] + d, groups[phase]))
            return carry

        lax.fori_loop(1, groups[phase], one, 0)

    barrier = pltpu.get_barrier_semaphore()
    for phase in range(2):
        each_peer(
            phase,
            lambda i, phase=phase: pl.semaphore_signal(
                barrier, inc=1, device_id=peer(phase, i), device_id_type=MESH
            ),
        )

    def spread(phase, src, buf, send, recv, unroll=False):
        def act(i):
            pltpu.make_async_remote_copy(
                src_ref=src,
                dst_ref=buf.at[me[phase]],
                send_sem=send,
                recv_sem=recv,
                device_id=peer(phase, i),
                device_id_type=MESH,
            ).start()

        each_peer(phase, act, unroll)

    def settle(phase, buf, sem):
        part = buf.at[pl.ds(0, groups[phase] - 1)]
        pltpu.make_async_copy(part, part, sem).wait()

    lane = lax.broadcasted_iota(jnp.int32, (1, COLS), 1)
    low = lane < C

    def columns(row_a, row_b):
        return to_cols(jnp.concatenate([row_a, row_b], axis=1))

    w = [pfn_w[f : f + 1, :] for f in range(9)]
    rows = [w[0] + w[4] + w[7], w[1] + w[5] + w[8], w[2] + w[6], w[3]] + w[4:9] + [w[8]]
    for k in range(0, 10, 2):
        pwc[k], pwc[k + 1] = columns(rows[k], rows[k + 1])

    half = lambda x, h: x[:, h * COLS : (h + 1) * COLS]
    slot = lax.broadcasted_iota(jnp.int32, (MAXP, PILL), 0)
    local_n = jnp.sum(counts[...].astype(F32))
    mean_tile = jnp.zeros((C, COLS), F32)
    for s in range(SW):
        n_row = counts[s : s + 1, :]
        n_f = n_row.astype(F32)
        ok = slot < n_row
        sums = [
            jnp.sum(jnp.where(ok, points[s, j], 0.0), axis=0, keepdims=True) for j in range(4)
        ]
        cell = cells[s : s + 1, :]
        col_pos = lax.rem(cell, 2 * COLS).astype(F32) * (1.0 / COLS) - 1.0
        row_pos = (cell // (2 * COLS)).astype(F32) * 0.25 - 1.0
        fixed = [sums[0] / n_f, sums[1] / n_f, sums[2] / n_f, col_pos, row_pos]
        for h in range(2):
            off = jnp.zeros((C, COLS), F32)
            for j in range(5):
                off = off - pwc[4 + j] * half(fixed[j], h)
            base[s, :, h * COLS : (h + 1) * COLS] = off
            acc = off * half(n_f, h)
            for j in range(4):
                acc = acc + pwc[j] * half(sums[j], h)
            mean_tile = mean_tile + acc
    local_mean = jnp.sum(mean_tile, axis=1, keepdims=True) / local_n

    pwc[9] = jnp.broadcast_to(local_mean, (C, COLS))
    for s in range(SW):
        base[s] = base[s] - wide(pwc[9], 2)

    grp = 16

    def channels(g, carry):
        at = pl.ds(pl.multiple_of(g * grp, grp), grp)
        wj = [pwc[j, at, :] for j in range(4)]

        def walk(k8, carry):
            tops, acc = list(carry[:-1]), carry[-1]
            first = pl.multiple_of(k8 * 8, 8)
            for s in range(SW):
                for h in range(2):
                    lanes = slice(h * COLS, (h + 1) * COLS)
                    off = base[s, at, lanes]
                    left = jnp.broadcast_to(counts[s : s + 1, lanes] - first, (grp, COLS))
                    pts = [points[s, j, pl.ds(first, 8), lanes] for j in range(4)]
                    for k in range(8):
                        value = off
                        for j in range(4):
                            value = value + wj[j] * pts[j][k : k + 1, :]
                        ok = left > k
                        top = jnp.where(ok, value, -3e38)
                        tops[2 * s + h] = jnp.maximum(tops[2 * s + h], top)
                        value = jnp.where(ok, value, 0.0)
                        acc = acc + value * value
            return (*tops, acc)

        start = [jnp.full((grp, COLS), -3e38, F32)] * (2 * SW)
        done = lax.fori_loop(0, MAXP // 8, walk, (*start, jnp.zeros((grp, COLS), F32)))
        for s in range(SW):
            for h in range(2):
                hmax[s, at, h * COLS : (h + 1) * COLS] = done[2 * s + h] + pwc[9, at, :]
        sq[at, :] = done[-1]
        return carry

    lax.fori_loop(0, C // grp, channels, 0)

    row = to_row(mean_tile, sq[...])
    row = jnp.where(low, row / local_n, row)
    payload = jnp.concatenate([row, jnp.full((1, COLS), local_n, F32)], axis=1)

    def merge_pfn(v):
        a, n = v[:, :, :COLS], v[:, :, COLS:]
        total = jnp.sum(n, axis=0)
        avg = jnp.sum(n * a, axis=0) / total
        dev = a - avg[None]
        spread_sq = jnp.sum(n * dev * dev, axis=0)
        both = jnp.where(low, avg, jnp.sum(a, axis=0) + pltpu.roll(spread_sq, C, 1))
        return jnp.concatenate([both, total], axis=1)

    pl.semaphore_wait(barrier, ga + gb - 2)
    p_src[0] = payload
    p_buf[0, me[0]] = payload
    spread(0, p_src.at[0], p_buf.at[0], p_send.at[0], p_recv.at[0], True)

    for s in range(SW):
        cell = cells[s : s + 1, :]
        r, c = cell // (2 * COLS), lax.rem(cell, 2 * COLS)
        spot = (
            (lax.rem(r, 2) * 2 + lax.rem(c, 2)) * PLANE + (r // 2) * COLS + c // 2
        )

        def fill(t, carry, s=s, spot=spot):
            ids = lax.broadcasted_iota(jnp.int32, (COLS, PILL), 0) + t * COLS
            hit = jnp.where(ids == spot, 1.0, 0.0)
            hot[s, pl.ds(pl.multiple_of(t * COLS, COLS), COLS), :] = hit.astype(BF16)
            return carry

        lax.fori_loop(0, 4 * PLANE // COLS, fill, 0)
    par[0], par[1] = columns(pfn_g[...], pfn_b[...])
    for l in range(LAYERS):
        par[2 + 2 * l], par[3 + 2 * l] = columns(bn_g[l : l + 1, :], bn_b[l : l + 1, :])

    pairs = 5

    def spread_rows(block, carry):
        for step in range(8):
            t = block * 8 + step
            at = pl.ds(pl.multiple_of(t * COLS, COLS), COLS)
            for k in range(pairs):
                a = conv_w[2 * k, :, at]
                b = conv_w[min(2 * k + 1, 8), :, at]
                w_raw[2 * t, k] = jnp.where(low, a, pltpu.roll(b, C, 1))
                w_raw[2 * t + 1, k] = jnp.where(low, pltpu.roll(a, C, 1), b)
        return carry

    lax.fori_loop(0, C // 16, spread_rows, 0)

    def taps_of(l, k):
        return w_raw[:, k, l, :]

    def turned(l, k):
        tile = taps_of(l, k).T
        return jnp.concatenate([tile[:C], tile[C:]], axis=1)

    def pair_lanes(k):
        return slice(k * COLS, min((k + 1) * COLS, K9))

    def forward_weights(l):
        for k in range(pairs):
            lanes = pair_lanes(k)
            tile = taps_of(l, k)[:, : lanes.stop - lanes.start]
            wf[l, :C, lanes], wf[l, C:, lanes] = split(tile)

    def backward_weights():
        for l in range(1, LAYERS):
            for k in range(pairs):
                lanes = pair_lanes(k)
                tile = turned(l, k)[:, : lanes.stop - lanes.start]
                wb[l, :C, lanes], wb[l, C:, lanes] = split(tile)
        w_bwd0 = jnp.concatenate([turned(0, k) for k in range(pairs)], axis=1)[:, :K9]
        tap = lax.broadcasted_iota(jnp.int32, (C, K9), 1) // C
        parity = jnp.where(tap // 3 == 1, 0, 2) + jnp.where(lax.rem(tap, 3) == 1, 0, 1)
        for ph in range(4):
            hi, lo = split(jnp.where(parity == ph, w_bwd0, 0.0))
            w0h[ph * C : (ph + 1) * C, :] = hi
            w0l[ph * C : (ph + 1) * C, :] = lo

    forward_weights(0)

    settle(0, p_buf.at[0], p_recv.at[0])
    payload = merge_pfn(p_buf[0, pl.ds(0, ga)])
    p_src[1] = payload
    p_buf[1, me[1]] = payload
    spread(1, p_src.at[1], p_buf.at[1], p_send.at[1], p_recv.at[1], True)
    for l in range(1, LAYERS):
        forward_weights(l)
    settle(1, p_buf.at[1], p_recv.at[1])
    payload = merge_pfn(p_buf[1, pl.ds(0, gb)])
    row, total = payload[:, :COLS], payload[:, COLS:]
    mean_c, inv_c = to_cols(jnp.where(low, row, lax.rsqrt(row / total + EPS)))
    scale = par[0] * inv_c

    for s in range(SW):
        pillar = jnp.concatenate(
            [
                jnp.maximum((half(hmax[s], h) - mean_c) * scale + par[1], 0.0)
                for h in range(2)
            ],
            axis=1,
        )
        hi, lo = split(pillar)
        both = jnp.concatenate([hi, lo], axis=0)
        lanes = slice(s * PLANE, (s + 1) * PLANE)
        for pr in range(2):
            for pc in range(2):
                ph = 2 * pr + pc
                plane = mmt(both, hot[s, ph * PLANE : (ph + 1) * PLANE, :])
                for b in (0, 2) if pc else (1,):
                    moved = col_shift(plane, -1 if b == 0 else 0).astype(BF16)
                    for a in (0, 2) if pr else (1,):
                        out = row_shift(moved, -1 if a == 0 else 0)
                        at = slice((3 * a + b) * C, (3 * a + b + 1) * C)
                        x9h[0, at, lanes] = out[:C]
                        x9l[0, at, lanes] = out[C:]

    def send_stat(rnd, phase, row):
        s_src[rnd, phase] = row
        s_buf[rnd, phase, me[phase]] = row
        spread(
            phase,
            s_src.at[rnd, phase],
            s_buf.at[rnd, phase],
            s_send.at[rnd, phase],
            s_recv.at[rnd, phase],
            True,
        )

    def take_stat(rnd, phase):
        settle(phase, s_buf.at[rnd, phase], s_recv.at[rnd, phase])
        return s_buf[rnd, phase, pl.ds(0, groups[phase])]

    def merge_norm(v, count):
        total = jnp.sum(v, axis=0)
        avg = total / v.shape[0]
        dev = v - avg[None]
        spread_sq = jnp.sum(dev * dev, axis=0) * count
        return jnp.where(low, avg, total + pltpu.roll(spread_sq, C, 1))

    def norm_layer(l, rnd, meanwhile=None):
        xh = x9h.at[l]
        xl = x9l.at[l]
        wide_z = mm(wf[l], xh[...])
        z = wide_z[:C] + wide_z[C:] + mm(wf[l, :C, :], xl[...])
        part = fold(z)
        m = jnp.sum(part, axis=1, keepdims=True) * (1.0 / POS)
        dev = z - m
        row = to_row(part, fold(dev * dev))
        send_stat(rnd, 0, jnp.where(low, row * (1.0 / POS), row))
        if meanwhile is not None:
            meanwhile()
        row = merge_norm(take_stat(rnd, 0), float(POS))
        send_stat(rnd, 1, row)
        row = merge_norm(take_stat(rnd, 1), float(POS * ga))
        mean_col, inv_col = to_cols(
            jnp.where(low, row, lax.rsqrt(row * (1.0 / (POS * devices)) + EPS))
        )
        normed = (z - wide(mean_col, POS // COLS)) * wide(inv_col, POS // COLS)
        gain, bias = par[2 + 2 * l], par[3 + 2 * l]
        y = wide(gain, POS // COLS) * normed + wide(bias, POS // COLS)
        act, slp = silu_parts(y)
        xhat[l] = normed
        slope[l] = slp
        par[10 + l] = gain * inv_col
        return act

    rows = C // (nx * ny)
    pad = jnp.zeros((C, 2 * LANES - K9), F32)

    def pieces(value):
        value = jnp.concatenate([value, pad], axis=1)
        for i in range(ga):
            r_at = (i % (nx * ny)) * rows
            l_at = (i // (nx * ny)) * LANES
            yield i, value[r_at : r_at + rows, l_at : l_at + LANES]

    def scatter(src, buf, send, recv):
        def act(i):
            pltpu.make_async_remote_copy(
                src_ref=src.at[i],
                dst_ref=buf.at[me[0]],
                send_sem=send,
                recv_sem=recv,
                device_id=peer(0, i),
                device_id_type=MESH,
            ).start()

        each_peer(0, act)
        buf[me[0]] = src[me[0]]

    def fixed_start():
        hi, lo = split(xhat[0])
        ones = jnp.ones((C, POS), BF16)
        first = mmt(jnp.concatenate([hi, lo, ones], axis=0), x9h[0])
        second = mmt(jnp.concatenate([hi, ones], axis=0), x9l[0])
        corr = first[:C] + first[C : 2 * C] + second[:C]
        plain = first[2 * C : 3 * C] + second[C : 2 * C]
        for i, part in pieces(corr):
            c_src[i, :rows, :] = part
        for i, part in pieces(plain):
            c_src[i, rows:, :] = part
        scatter(c_src, c_buf, c_send.at[0], c_recv.at[0])

    def fixed_cross():
        settle(0, c_buf, c_recv.at[0])
        part = jnp.sum(c_buf[...], axis=0)
        cx_src[...] = part
        cx_buf[me[1]] = part
        spread(1, cx_src, cx_buf, c_send.at[1], c_recv.at[1])

    store_taps(norm_layer(0, 0, backward_weights), x9h.at[1], x9l.at[1], 1)

    def middle(l, carry):
        def meanwhile():
            pl.when(l == 1)(fixed_start)
            pl.when(l == 2)(fixed_cross)

        store_taps(norm_layer(l, l, meanwhile), x9h.at[l + 1], x9l.at[l + 1], 1)
        return carry

    lax.fori_loop(1, LAYERS - 1, middle, 0)
    act = norm_layer(LAYERS - 1, LAYERS - 1)
    for s in range(SW):
        for i in range(ROWS):
            at = s * PLANE + i * COLS
            features[s, :, i, :] = act[:, at : at + COLS]
            u_ref[:, at : at + COLS] = cot[s, :, i, :]

    def grad_start(l, gh=None, gl=None):
        if gh is None:
            gh, gl = g9h[4 * C : 5 * C, :], g9l[4 * C : 5 * C, :]
        both = jnp.concatenate([gh, gl], axis=0)
        first = mmt(both, x9h[l])
        for i, part in pieces(first[:C] + first[C:] + mmt(gh, x9l[l])):
            dw[l, i] = part
        scatter(dw.at[l], rs_buf.at[l], g_send.at[l, 0], g_recv.at[l, 0])

    def grad_cross(l):
        settle(0, rs_buf.at[l], g_recv.at[l, 0])
        part = jnp.sum(rs_buf[l], axis=0)
        x_src[l] = part
        x_buf[l, me[1]] = part
        spread(1, x_src.at[l], x_buf.at[l], g_send.at[l, 1], g_recv.at[l, 1])

    def grad_back(l, finish=None):
        settle(1, x_buf.at[l], g_recv.at[l, 1])
        part = jnp.sum(x_buf[l], axis=0)
        if finish is not None:
            part = finish(part)
        for k in range(LANES // COLS):
            tile = part[:, k * COLS : (k + 1) * COLS]
            swapped = pltpu.roll(tile, C, 1)
            for p in range(rows // 2):
                even, odd = slice(2 * p, 2 * p + 1), slice(2 * p + 1, 2 * p + 2)
                lanes = slice(p * COLS, (p + 1) * COLS)
                first = jnp.where(low, tile[even], swapped[odd])
                second = jnp.where(low, swapped[even], tile[odd])
                ag_src[l, 2 * k : 2 * k + 1, lanes] = first
                ag_src[l, 2 * k + 1 : 2 * k + 2, lanes] = second
        spread(0, ag_src.at[l], full.at[l], g_send.at[l, 2], g_recv.at[l, 2])
        full[l, me[0]] = ag_src[l]

    total_m = 1.0 / (POS * devices)

    def sums_start(l, rnd):
        gy = u_ref[...] * slope[l]
        gy_ref[...] = gy
        send_stat(rnd, 0, to_row(fold(gy), fold(gy * xhat[l])))

    def sums_cross(rnd):
        send_stat(rnd, 1, jnp.sum(take_stat(rnd, 0), axis=0))

    def sums_end(l, rnd):
        row = jnp.sum(take_stat(rnd, 1), axis=0)
        norm_out[1, pl.ds(l, 1), :] = row[:, :C]
        norm_out[0, pl.ds(l, 1), :] = pltpu.roll(row, C, 1)[:, :C]
        return to_cols(row * total_m)

    def grad_z(l, dy, dx):
        n = POS // COLS
        return wide(par[10 + l], n) * (gy_ref[...] - wide(dy, n) - xhat[l] * wide(dx, n))

    def back(t, carry):
        l = LAYERS - 1 - t
        sums_start(l, LAYERS + t)

        @pl.when(t > 0)
        def _():
            grad_start(l + 1)

        @pl.when(t > 1)
        def _():
            grad_back(l + 2)

        sums_cross(LAYERS + t)

        @pl.when(t > 0)
        def _():
            grad_cross(l + 1)

        store_taps(grad_z(l, *sums_end(l, LAYERS + t)), g9h, g9l, -1)
        first = mm(wb[l], g9h[...])
        u_ref[...] = first[:C] + first[C:] + mm(wb[l, :C, :], g9l[...])
        return carry

    lax.fori_loop(0, LAYERS - 1, back, 0)
    rnd = 2 * LAYERS - 1
    sums_start(0, rnd)
    grad_start(0, *split(gy_ref[...]))
    grad_start(1)
    grad_back(2)
    sums_cross(rnd)
    grad_cross(0)
    grad_cross(1)
    settle(1, cx_buf, c_recv.at[1])
    fixed = jnp.sum(cx_buf[...], axis=0)
    dy, dx = sums_end(0, rnd)
    for k, tile in enumerate((dy, dx, par[10])):
        for q in range(nx * ny):
            trio[k, q] = tile[q * rows : (q + 1) * rows]

    def finish(part):
        dy_m, dx_m, k_m = [wide(trio[k, mine], LANES // COLS) for k in range(3)]
        return k_m * (part - fixed[rows:] * dy_m - fixed[:rows] * dx_m)

    grad_back(0, finish)
    grad_back(1)
    gz = grad_z(0, dy, dx)
    for b in range(3):
        hi, lo = split(col_shift(gz, 1 if b == 0 else 0))
        for a in range(3):
            at = slice((3 * a + b) * C, (3 * a + b + 1) * C)
            g9h[at, :] = row_shift(hi, 1 if a == 0 else 0)
            g9l[at, :] = row_shift(lo, 1 if a == 0 else 0)
    u0 = mm(w0h[...], g9h[...]) + mm(w0l[...], g9h[...]) + mm(w0h[...], g9l[...])
    for s in range(SW):
        acc = jnp.zeros((2 * C, PILL), F32)
        for ph in range(4):
            hi, lo = split(u0[ph * C : (ph + 1) * C, s * PLANE : (s + 1) * PLANE])
            both = jnp.concatenate([hi, lo], axis=0)
            acc = acc + mm(both, hot[s, ph * PLANE : (ph + 1) * PLANE, :])
        pillar_out[s] = acc[:C] + acc[C:]

    for phase in range(2):
        settle(phase, p_buf.at[phase], p_send.at[phase])
        for r in range(2 * LAYERS):
            settle(phase, s_buf.at[r, phase], s_send.at[r, phase])
    settle(0, c_buf, c_send.at[0])
    settle(1, cx_buf, c_send.at[1])
    for l in range(LAYERS):
        settle(0, rs_buf.at[l], g_send.at[l, 0])
        settle(1, x_buf.at[l], g_send.at[l, 1])
        settle(0, full.at[l], g_send.at[l, 2])
        settle(0, full.at[l], g_recv.at[l, 2])
        span = rows * C
        for i in range(ga):
            lanes = slice((i % (nx * ny)) * span, (i % (nx * ny) + 1) * span)
            first = (i // (nx * ny)) * (LANES // C)
            count = min(LANES // C, 9 - first)
            grads_out[first : first + count, l, lanes] = full[l, i, :count, :]


def deliver_kernel(*refs):
    *refs, sem = refs
    half = len(refs) // 2
    copies = [
        pltpu.make_async_copy(refs[k], refs[half + k], sem.at[k]) for k in range(half)
    ]
    for copy in copies:
        copy.start()
    for copy in copies:
        copy.wait()


def deliver(arrays):
    return pl.pallas_call(
        deliver_kernel,
        out_shape=tuple(jax.ShapeDtypeStruct(a.shape, a.dtype) for a in arrays),
        in_specs=[pl.BlockSpec(memory_space=pltpu.VMEM)] * len(arrays),
        out_specs=(pl.BlockSpec(memory_space=pl.ANY),) * len(arrays),
        scratch_shapes=[pltpu.SemaphoreType.DMA((len(arrays),))],
        compiler_params=pltpu.CompilerParams(vmem_limit_bytes=VLIM * 2**20),
    )(*arrays)


def solution(mesh, ny=NY, nz=NZ):
    nx = mesh.shape["rack"] // CORES
    ga, gb = CORES * nx * ny, nz
    gmax = max(ga, gb)
    rows = C // (nx * ny)

    def per_device(
        points, counts, cells, pfn_w, pfn_g, pfn_b, conv_w, bn_g, bn_b, cotangent
    ):
        vmem = pl.BlockSpec(memory_space=pltpu.VMEM)
        dma = pltpu.SemaphoreType.DMA
        out = pl.pallas_call(
            functools.partial(step_kernel, (nx, ny, nz)),
            out_shape=(
                jax.ShapeDtypeStruct((SW, C, ROWS, COLS), F32),
                jax.ShapeDtypeStruct((9, LAYERS, C * C), F32),
                jax.ShapeDtypeStruct((2, LAYERS, C), F32),
                jax.ShapeDtypeStruct((SW, C, PILL), F32),
            ),
            in_specs=[vmem] * 10,
            out_specs=(vmem,) * 4,
            scratch_shapes=[
                pltpu.VMEM((LAYERS, K9, POS), BF16),
                pltpu.VMEM((LAYERS, K9, POS), BF16),
                pltpu.VMEM((K9, POS), BF16),
                pltpu.VMEM((K9, POS), BF16),
                pltpu.VMEM((SW, 4 * PLANE, PILL), BF16),
                pltpu.VMEM((LAYERS, C, POS), F32),
                pltpu.VMEM((LAYERS, C, POS), F32),
                pltpu.VMEM((LAYERS, 2 * C, K9), BF16),
                pltpu.VMEM((LAYERS, 2 * C, K9), BF16),
                pltpu.VMEM((4 * C, K9), BF16),
                pltpu.VMEM((4 * C, K9), BF16),
                pltpu.VMEM((C, 5, LAYERS, COLS), F32),
                pltpu.VMEM((14, C, COLS), F32),
                pltpu.VMEM((10, C, COLS), F32),
                pltpu.VMEM((SW, C, PILL), F32),
                pltpu.VMEM((SW, C, PILL), F32),
                pltpu.VMEM((C, COLS), F32),
                pltpu.VMEM((C, POS), F32),
                pltpu.VMEM((C, POS), F32),
                pltpu.VMEM((2, 1, 2 * COLS), F32),
                pltpu.VMEM((2, gmax, 1, 2 * COLS), F32),
                pltpu.VMEM((2 * LAYERS, 2, 1, COLS), F32),
                pltpu.VMEM((2 * LAYERS, 2, gmax, 1, COLS), F32),
                pltpu.VMEM((LAYERS, ga, rows, LANES), F32),
                pltpu.VMEM((LAYERS, ga, rows, LANES), F32),
                pltpu.VMEM((LAYERS, rows, LANES), F32),
                pltpu.VMEM((LAYERS, gb, rows, LANES), F32),
                pltpu.VMEM((LAYERS, LANES // C, rows * C), F32),
                pltpu.VMEM((LAYERS, ga, LANES // C, rows * C), F32),
                pltpu.VMEM((ga, 2 * rows, LANES), F32),
                pltpu.VMEM((ga, 2 * rows, LANES), F32),
                pltpu.VMEM((2 * rows, LANES), F32),
                pltpu.VMEM((gb, 2 * rows, LANES), F32),
                pltpu.VMEM((3, ga // CORES, rows, COLS), F32),
                dma((2,)),
                dma((2,)),
                dma((2,)),
                dma((2,)),
                dma((2 * LAYERS, 2)),
                dma((2 * LAYERS, 2)),
                dma((LAYERS, 3)),
                dma((LAYERS, 3)),
            ],
            compiler_params=pltpu.CompilerParams(
                collective_id=0, has_side_effects=True, vmem_limit_bytes=VLIM * 2**20
            ),
        )(
            points,
            counts,
            cells,
            pfn_w,
            pfn_g.reshape(1, C),
            pfn_b.reshape(1, C),
            conv_w.transpose(1, 0, 2),
            bn_g,
            bn_b,
            cotangent,
        )
        features, grads, norm_grads, pillar_grad = deliver(out)
        return features, grads.transpose(1, 0, 2), norm_grads, pillar_grad

    split_all = ("rack", "chip")
    return jax.shard_map(
        per_device,
        mesh=mesh,
        in_specs=(
            P(split_all, None, None, None),
            P(split_all, None),
            P(split_all, None),
            P(),
            P(),
            P(),
            P(),
            P(),
            P(),
            P(split_all, None, None, None),
        ),
        out_specs=(
            P(split_all, None, None, None),
            P(),
            P(),
            P(split_all, None, None),
        ),
        check_vma=False,
    )
```

```python
import functools

import jax
import jax.numpy as jnp
from jax import lax
from jax.experimental import pallas as pl
from jax.experimental.pallas import tpu as pltpu
from jax.sharding import PartitionSpec as P

C = 64
MAXP = 32
LAYERS = 4
PILL = 256
COLS = 128
ROWS = 4
SW = 2
PLANE = ROWS * COLS
POS = SW * PLANE
K9 = 9 * C
EPS = 1e-05
CORES = 2
NZ = 8
NY = 4
LANES = 384
VLIM = 60
MESH = pl.DeviceIdType.MESH
F32 = jnp.float32
BF16 = jnp.bfloat16


def split(x):
    hi = x.astype(BF16)
    return hi, (x - hi.astype(F32)).astype(BF16)


def mm(a, b):
    return lax.dot_general(a, b, (((1,), (0,)), ((), ())), preferred_element_type=F32)


def mmt(a, b):
    return lax.dot_general(a, b, (((1,), (1,)), ((), ())), preferred_element_type=F32)


def fold(x):
    parts = [x[:, t * COLS : (t + 1) * COLS] for t in range(x.shape[1] // COLS)]
    while len(parts) > 1:
        parts = [parts[t] + parts[t + 1] for t in range(0, len(parts), 2)]
    return parts[0]


def wide(tile, n):
    return jnp.concatenate([tile] * n, axis=1)


def to_row(a, b):
    return jnp.sum(jnp.concatenate([a, b], axis=0).T, axis=0, keepdims=True)


def to_cols(row):
    full = jnp.broadcast_to(row, (2 * C, COLS)).T
    return full[:C], full[C:]


def col_shift(x, step):
    if step == 0:
        return x
    lane = lax.broadcasted_iota(jnp.int32, (x.shape[0], COLS), 1)
    edge = lane == (COLS - 1 if step > 0 else 0)
    turn = COLS - 1 if step > 0 else 1
    tiles = []
    for t in range(x.shape[1] // COLS):
        tile = pltpu.roll(x[:, t * COLS : (t + 1) * COLS], turn, 1)
        tiles.append(jnp.where(edge, 0.0, tile))
    return jnp.concatenate(tiles, axis=1)


def row_shift(x, step):
    if step == 0:
        return x
    none = jnp.zeros((x.shape[0], COLS), x.dtype)
    parts = []
    for s in range(x.shape[1] // PLANE):
        base = s * PLANE
        if step > 0:
            parts += [x[:, base + COLS : base + PLANE], none]
        else:
            parts += [none, x[:, base : base + PLANE - COLS]]
    return jnp.concatenate(parts, axis=1)


def store_taps(x, hi_ref, lo_ref, sign):
    for b in range(3):
        hi, lo = split(col_shift(x, sign * (b - 1)))
        for a in range(3):
            at = pl.ds((3 * a + b) * C, C)
            hi_ref[at, :] = row_shift(hi, sign * (a - 1))
            lo_ref[at, :] = row_shift(lo, sign * (a - 1))


def silu_parts(y):
    sg = 1.0 / (1.0 + jnp.exp(-y))
    return y * sg, sg * (1.0 + y * (1.0 - sg))


def step_kernel(
    size,
    points,
    counts,
    cells,
    pfn_w,
    pfn_g,
    pfn_b,
    conv_w,
    bn_g,
    bn_b,
    cot,
    features,
    grads_out,
    norm_out,
    pillar_out,
    x9h,
    x9l,
    g9h,
    g9l,
    hot,
    xhat,
    slope,
    wf,
    wb,
    w0h,
    w0l,
    w_raw,
    par,
    pwc,
    hmax,
    base,
    sq,
    u_ref,
    gy_ref,
    p_src,
    p_buf,
    s_src,
    s_buf,
    dw,
    rs_buf,
    x_src,
    x_buf,
    ag_src,
    full,
    c_src,
    c_buf,
    cx_src,
    cx_buf,
    trio,
    zh,
    zl,
    d_src,
    d_buf,
    dx_src,
    dx_buf,
    dg_src,
    d_full,
    q_src,
    q_buf,
    c_send,
    c_recv,
    d_send,
    d_recv,
    q_send,
    q_recv,
    p_send,
    p_recv,
    s_send,
    s_recv,
    g_send,
    g_recv,
):
    nx, ny, nz = size
    ga, gb = CORES * nx * ny, nz
    devices = ga * gb
    rack = lax.axis_index("rack")
    chip = lax.axis_index("chip")
    core = lax.rem(rack, CORES)
    my_x = rack // CORES
    my_z = lax.rem(chip, nz)
    my_y = chip // nz
    mine = my_x * ny + my_y
    me = (core * (nx * ny) + mine, my_z)
    groups = (ga, gb)

    def peer(phase, i):
        if phase == 0:
            at = lax.rem(i, nx * ny)
            return ((at // ny) * CORES + i // (nx * ny), lax.rem(at, ny) * nz + my_z)
        return (rack, my_y * nz + i)

    def each_peer(phase, act, unroll=False):
        if unroll:
            for d in range(1, groups[phase]):
                act(lax.rem(me[phase] + d, groups[phase]))
            return

        def one(d, carry):
            act(lax.rem(me[phase] + d, groups[phase]))
            return carry

        lax.fori_loop(1, groups[phase], one, 0)

    barrier = pltpu.get_barrier_semaphore()
    for phase in range(2):
        each_peer(
            phase,
            lambda i, phase=phase: pl.semaphore_signal(
                barrier, inc=1, device_id=peer(phase, i), device_id_type=MESH
            ),
        )

    def spread(phase, src, buf, send, recv, unroll=False):
        def act(i):
            pltpu.make_async_remote_copy(
                src_ref=src,
                dst_ref=buf.at[me[phase]],
                send_sem=send,
                recv_sem=recv,
                device_id=peer(phase, i),
                device_id_type=MESH,
            ).start()

        each_peer(phase, act, unroll)

    def settle(phase, buf, sem):
        part = buf.at[pl.ds(0, groups[phase] - 1)]
        pltpu.make_async_copy(part, part, sem).wait()

    lane = lax.broadcasted_iota(jnp.int32, (1, COLS), 1)
    low = lane < C

    def columns(row_a, row_b):
        return to_cols(jnp.concatenate([row_a, row_b], axis=1))

    w = [pfn_w[f : f + 1, :] for f in range(9)]
    rows = [w[0] + w[4] + w[7], w[1] + w[5] + w[8], w[2] + w[6], w[3]] + w[4:9] + [w[8]]
    for k in range(0, 10, 2):
        pwc[k], pwc[k + 1] = columns(rows[k], rows[k + 1])

    half = lambda x, h: x[:, h * COLS : (h + 1) * COLS]
    slot = lax.broadcasted_iota(jnp.int32, (MAXP, PILL), 0)
    local_n = jnp.sum(counts[...].astype(F32))
    mean_tile = jnp.zeros((C, COLS), F32)
    for s in range(SW):
        n_row = counts[s : s + 1, :]
        n_f = n_row.astype(F32)
        ok = slot < n_row
        sums = [
            jnp.sum(jnp.where(ok, points[s, j], 0.0), axis=0, keepdims=True) for j in range(4)
        ]
        cell = cells[s : s + 1, :]
        col_pos = lax.rem(cell, 2 * COLS).astype(F32) * (1.0 / COLS) - 1.0
        row_pos = (cell // (2 * COLS)).astype(F32) * 0.25 - 1.0
        fixed = [sums[0] / n_f, sums[1] / n_f, sums[2] / n_f, col_pos, row_pos]
        for h in range(2):
            off = jnp.zeros((C, COLS), F32)
            for j in range(5):
                off = off - pwc[4 + j] * half(fixed[j], h)
            base[s, :, h * COLS : (h + 1) * COLS] = off
            acc = off * half(n_f, h)
            for j in range(4):
                acc = acc + pwc[j] * half(sums[j], h)
            mean_tile = mean_tile + acc
    local_mean = jnp.sum(mean_tile, axis=1, keepdims=True) / local_n

    pwc[9] = jnp.broadcast_to(local_mean, (C, COLS))
    for s in range(SW):
        base[s] = base[s] - wide(pwc[9], 2)

    grp = 16

    def channels(g, carry):
        at = pl.ds(pl.multiple_of(g * grp, grp), grp)
        wj = [pwc[j, at, :] for j in range(4)]

        def walk(k8, carry):
            tops, acc = list(carry[:-1]), carry[-1]
            first = pl.multiple_of(k8 * 8, 8)
            for s in range(SW):
                for h in range(2):
                    lanes = slice(h * COLS, (h + 1) * COLS)
                    off = base[s, at, lanes]
                    left = jnp.broadcast_to(counts[s : s + 1, lanes] - first, (grp, COLS))
                    pts = [points[s, j, pl.ds(first, 8), lanes] for j in range(4)]
                    for k in range(8):
                        value = off
                        for j in range(4):
                            value = value + wj[j] * pts[j][k : k + 1, :]
                        ok = left > k
                        top = jnp.where(ok, value, -3e38)
                        tops[2 * s + h] = jnp.maximum(tops[2 * s + h], top)
                        value = jnp.where(ok, value, 0.0)
                        acc = acc + value * value
            return (*tops, acc)

        start = [jnp.full((grp, COLS), -3e38, F32)] * (2 * SW)
        done = lax.fori_loop(0, MAXP // 8, walk, (*start, jnp.zeros((grp, COLS), F32)))
        for s in range(SW):
            for h in range(2):
                hmax[s, at, h * COLS : (h + 1) * COLS] = done[2 * s + h] + pwc[9, at, :]
        sq[at, :] = done[-1]
        return carry

    lax.fori_loop(0, C // grp, channels, 0)

    row = to_row(mean_tile, sq[...])
    row = jnp.where(low, row / local_n, row)
    payload = jnp.concatenate([row, jnp.full((1, COLS), local_n, F32)], axis=1)

    def merge_pfn(v):
        a, n = v[:, :, :COLS], v[:, :, COLS:]
        total = jnp.sum(n, axis=0)
        avg = jnp.sum(n * a, axis=0) / total
        dev = a - avg[None]
        spread_sq = jnp.sum(n * dev * dev, axis=0)
        both = jnp.where(low, avg, jnp.sum(a, axis=0) + pltpu.roll(spread_sq, C, 1))
        return jnp.concatenate([both, total], axis=1)

    pl.semaphore_wait(barrier, ga + gb - 2)
    p_src[0] = payload
    p_buf[0, me[0]] = payload
    spread(0, p_src.at[0], p_buf.at[0], p_send.at[0], p_recv.at[0], True)

    for s in range(SW):
        cell = cells[s : s + 1, :]
        r, c = cell // (2 * COLS), lax.rem(cell, 2 * COLS)
        spot = (
            (lax.rem(r, 2) * 2 + lax.rem(c, 2)) * PLANE + (r // 2) * COLS + c // 2
        )

        def fill(t, carry, s=s, spot=spot):
            ids = lax.broadcasted_iota(jnp.int32, (COLS, PILL), 0) + t * COLS
            hit = jnp.where(ids == spot, 1.0, 0.0)
            hot[s, pl.ds(pl.multiple_of(t * COLS, COLS), COLS), :] = hit.astype(BF16)
            return carry

        lax.fori_loop(0, 4 * PLANE // COLS, fill, 0)
    par[0], par[1] = columns(pfn_g[...], pfn_b[...])
    for l in range(LAYERS):
        par[2 + 2 * l], par[3 + 2 * l] = columns(bn_g[l : l + 1, :], bn_b[l : l + 1, :])

    pairs = 5

    def spread_rows(block, carry):
        for step in range(8):
            t = block * 8 + step
            at = pl.ds(pl.multiple_of(t * COLS, COLS), COLS)
            for k in range(pairs):
                a = conv_w[2 * k, :, at]
                b = conv_w[min(2 * k + 1, 8), :, at]
                w_raw[2 * t, k] = jnp.where(low, a, pltpu.roll(b, C, 1))
                w_raw[2 * t + 1, k] = jnp.where(low, pltpu.roll(a, C, 1), b)
        return carry

    lax.fori_loop(0, C // 16, spread_rows, 0)

    def taps_of(l, k):
        return w_raw[:, k, l, :]

    def turned(l, k):
        tile = taps_of(l, k).T
        return jnp.concatenate([tile[:C], tile[C:]], axis=1)

    def pair_lanes(k):
        return slice(k * COLS, min((k + 1) * COLS, K9))

    def forward_weights(l):
        for k in range(pairs):
            lanes = pair_lanes(k)
            tile = taps_of(l, k)[:, : lanes.stop - lanes.start]
            wf[l, :C, lanes], wf[l, C:, lanes] = split(tile)

    def backward_weights():
        for l in range(1, LAYERS):
            for k in range(pairs):
                lanes = pair_lanes(k)
                tile = turned(l, k)[:, : lanes.stop - lanes.start]
                wb[l, :C, lanes], wb[l, C:, lanes] = split(tile)
        w_bwd0 = jnp.concatenate([turned(0, k) for k in range(pairs)], axis=1)[:, :K9]
        tap = lax.broadcasted_iota(jnp.int32, (C, K9), 1) // C
        parity = jnp.where(tap // 3 == 1, 0, 2) + jnp.where(lax.rem(tap, 3) == 1, 0, 1)
        for ph in range(4):
            hi, lo = split(jnp.where(parity == ph, w_bwd0, 0.0))
            w0h[ph * C : (ph + 1) * C, :] = hi
            w0l[ph * C : (ph + 1) * C, :] = lo

    forward_weights(0)

    settle(0, p_buf.at[0], p_recv.at[0])
    payload = merge_pfn(p_buf[0, pl.ds(0, ga)])
    p_src[1] = payload
    p_buf[1, me[1]] = payload
    spread(1, p_src.at[1], p_buf.at[1], p_send.at[1], p_recv.at[1], True)
    for l in range(1, LAYERS):
        forward_weights(l)
    settle(1, p_buf.at[1], p_recv.at[1])
    payload = merge_pfn(p_buf[1, pl.ds(0, gb)])
    row, total = payload[:, :COLS], payload[:, COLS:]
    mean_c, inv_c = to_cols(jnp.where(low, row, lax.rsqrt(row / total + EPS)))
    scale = par[0] * inv_c

    for s in range(SW):
        pillar = jnp.concatenate(
            [
                jnp.maximum((half(hmax[s], h) - mean_c) * scale + par[1], 0.0)
                for h in range(2)
            ],
            axis=1,
        )
        hi, lo = split(pillar)
        both = jnp.concatenate([hi, lo], axis=0)
        lanes = slice(s * PLANE, (s + 1) * PLANE)
        for pr in range(2):
            for pc in range(2):
                ph = 2 * pr + pc
                plane = mmt(both, hot[s, ph * PLANE : (ph + 1) * PLANE, :])
                for b in (0, 2) if pc else (1,):
                    moved = col_shift(plane, -1 if b == 0 else 0).astype(BF16)
                    for a in (0, 2) if pr else (1,):
                        out = row_shift(moved, -1 if a == 0 else 0)
                        at = slice((3 * a + b) * C, (3 * a + b + 1) * C)
                        x9h[0, at, lanes] = out[:C]
                        x9l[0, at, lanes] = out[C:]

    def send_stat(rnd, phase, row):
        s_src[rnd, phase] = row
        s_buf[rnd, phase, me[phase]] = row
        spread(
            phase,
            s_src.at[rnd, phase],
            s_buf.at[rnd, phase],
            s_send.at[rnd, phase],
            s_recv.at[rnd, phase],
            True,
        )

    def take_stat(rnd, phase):
        settle(phase, s_buf.at[rnd, phase], s_recv.at[rnd, phase])
        return s_buf[rnd, phase, pl.ds(0, groups[phase])]

    def merge_norm(v, count):
        total = jnp.sum(v, axis=0)
        avg = total / v.shape[0]
        dev = v - avg[None]
        spread_sq = jnp.sum(dev * dev, axis=0) * count
        return jnp.where(low, avg, total + pltpu.roll(spread_sq, C, 1))

    def norm_layer(l, rnd, meanwhile=None, later=None):
        xh = x9h.at[l]
        xl = x9l.at[l]
        wide_z = mm(wf[l], xh[...])
        z = wide_z[:C] + wide_z[C:] + mm(wf[l, :C, :], xl[...])
        part = fold(z)
        m = jnp.sum(part, axis=1, keepdims=True) * (1.0 / POS)
        dev = z - m
        row = to_row(part, fold(dev * dev))
        send_stat(rnd, 0, jnp.where(low, row * (1.0 / POS), row))
        if meanwhile is not None:
            meanwhile()
        row = merge_norm(take_stat(rnd, 0), float(POS))
        send_stat(rnd, 1, row)
        if later is not None:
            later()
        row = merge_norm(take_stat(rnd, 1), float(POS * ga))
        mean_col, inv_col = to_cols(
            jnp.where(low, row, lax.rsqrt(row * (1.0 / (POS * devices)) + EPS))
        )
        normed = (z - wide(mean_col, POS // COLS)) * wide(inv_col, POS // COLS)
        gain, bias = par[2 + 2 * l], par[3 + 2 * l]
        y = wide(gain, POS // COLS) * normed + wide(bias, POS // COLS)
        act, slp = silu_parts(y)
        xhat[l] = normed
        slope[l] = slp
        par[10 + l] = gain * inv_col
        return act

    rows = C // (nx * ny)
    pad = jnp.zeros((C, 2 * LANES - K9), F32)

    def pieces(value):
        value = jnp.concatenate([value, pad], axis=1)
        for i in range(ga):
            r_at = (i % (nx * ny)) * rows
            l_at = (i // (nx * ny)) * LANES
            yield i, value[r_at : r_at + rows, l_at : l_at + LANES]

    def scatter(src, buf, send, recv):
        def act(i):
            pltpu.make_async_remote_copy(
                src_ref=src.at[i],
                dst_ref=buf.at[me[0]],
                send_sem=send,
                recv_sem=recv,
                device_id=peer(0, i),
                device_id_type=MESH,
            ).start()

        each_peer(0, act)
        buf[me[0]] = src[me[0]]

    def fixed_start():
        hi, lo = split(xhat[0])
        ones = jnp.ones((C, POS), BF16)
        first = mmt(jnp.concatenate([hi, lo, ones], axis=0), x9h[0])
        second = mmt(jnp.concatenate([hi, ones], axis=0), x9l[0])
        corr = first[:C] + first[C : 2 * C] + second[:C]
        plain = first[2 * C : 3 * C] + second[C : 2 * C]
        for i, part in pieces(corr):
            c_src[i, :rows, :] = part
        for i, part in pieces(plain):
            c_src[i, rows:, :] = part
        scatter(c_src, c_buf, c_send.at[0], c_recv.at[0])

    def fixed_cross():
        settle(0, c_buf, c_recv.at[0])
        part = jnp.sum(c_buf[...], axis=0)
        cx_src[...] = part
        cx_buf[me[1]] = part
        spread(1, cx_src, cx_buf, c_send.at[1], c_recv.at[1])

    store_taps(norm_layer(0, 0, backward_weights), x9h.at[1], x9l.at[1], 1)

    def middle(l, carry):
        def meanwhile():
            pl.when(l == 1)(fixed_start)
            pl.when(l == 2)(fixed_cross)

        store_taps(norm_layer(l, l, meanwhile), x9h.at[l + 1], x9l.at[l + 1], 1)
        return carry

    lax.fori_loop(1, LAYERS - 1, middle, 0)
    part_d = 2 * C // ga

    def pair_start():
        q = jnp.concatenate([slope[1], slope[1] * xhat[1]], axis=0)
        qh, ql = split(q)
        both = jnp.concatenate([qh, ql], axis=0)
        weight = wb[2, :C, :].astype(F32) + wb[2, C:, :].astype(F32)
        weight = jnp.concatenate([weight, weight], axis=0)

        def per_channel(e):
            p = e * weight
            t = p[:, :COLS]
            for k in range(1, 4):
                t = t + p[:, k * COLS : (k + 1) * COLS]
            return t[:, :C] + t[:, C:] + p[:, 4 * COLS :]

        store_taps(xhat[2], g9h, g9l, -1)
        e = mmt(both, g9h[...])
        by_normed = per_channel(e[: 2 * C] + e[2 * C :] + mmt(qh, g9l[...]))
        store_taps(jnp.ones((C, POS), F32), g9h, g9l, -1)
        e = mmt(both, g9h[...])
        by_one = per_channel(e[: 2 * C] + e[2 * C :])
        factors = jnp.concatenate([by_one, by_normed], axis=1).T
        for i in range(ga):
            d_src[i] = factors[i * part_d : (i + 1) * part_d]
        scatter(d_src, d_buf, d_send.at[0], d_recv.at[0])

    def pair_cross():
        settle(0, d_buf, d_recv.at[0])
        part = jnp.sum(d_buf[...], axis=0)
        dx_src[...] = part
        dx_buf[me[1]] = part
        spread(1, dx_src, dx_buf, d_send.at[1], d_recv.at[1])

    def pair_back():
        settle(1, dx_buf, d_recv.at[1])
        part = jnp.sum(dx_buf[...], axis=0)
        dg_src[...] = part
        spread(0, dg_src, d_full, d_send.at[2], d_recv.at[2])
        d_full[me[0]] = part

    act = norm_layer(LAYERS - 1, LAYERS - 1, pair_start, pair_cross)
    for s in range(SW):
        for i in range(ROWS):
            at = s * PLANE + i * COLS
            features[s, :, i, :] = act[:, at : at + COLS]
            u_ref[:, at : at + COLS] = cot[s, :, i, :]

    def grad_start(l, gh=None, gl=None):
        if gh is None:
            gh, gl = zh[l], zl[l]
        both = jnp.concatenate([gh, gl], axis=0)
        first = mmt(both, x9h[l])
        for i, part in pieces(first[:C] + first[C:] + mmt(gh, x9l[l])):
            dw[l, i] = part
        scatter(dw.at[l], rs_buf.at[l], g_send.at[l, 0], g_recv.at[l, 0])

    def grad_cross(l):
        settle(0, rs_buf.at[l], g_recv.at[l, 0])
        part = jnp.sum(rs_buf[l], axis=0)
        x_src[l] = part
        x_buf[l, me[1]] = part
        spread(1, x_src.at[l], x_buf.at[l], g_send.at[l, 1], g_recv.at[l, 1])

    def grad_back(l, finish=None):
        settle(1, x_buf.at[l], g_recv.at[l, 1])
        part = jnp.sum(x_buf[l], axis=0)
        if finish is not None:
            part = finish(part)
        for k in range(LANES // COLS):
            tile = part[:, k * COLS : (k + 1) * COLS]
            swapped = pltpu.roll(tile, C, 1)
            for p in range(rows // 2):
                even, odd = slice(2 * p, 2 * p + 1), slice(2 * p + 1, 2 * p + 2)
                lanes = slice(p * COLS, (p + 1) * COLS)
                first = jnp.where(low, tile[even], swapped[odd])
                second = jnp.where(low, swapped[even], tile[odd])
                ag_src[l, 2 * k : 2 * k + 1, lanes] = first
                ag_src[l, 2 * k + 1 : 2 * k + 2, lanes] = second
        spread(0, ag_src.at[l], full.at[l], g_send.at[l, 2], g_recv.at[l, 2])
        full[l, me[0]] = ag_src[l]

    total_m = 1.0 / (POS * devices)

    def sums_start(l, rnd):
        gy = u_ref[...] * slope[l]
        gy_ref[...] = gy
        send_stat(rnd, 0, to_row(fold(gy), fold(gy * xhat[l])))

    def sums_cross(rnd):
        send_stat(rnd, 1, jnp.sum(take_stat(rnd, 0), axis=0))

    def sums_end(l, rnd):
        return norms_done(l, jnp.sum(take_stat(rnd, 1), axis=0))

    def norms_done(l, row):
        norm_out[1, l : l + 1, :] = row[:, :C]
        norm_out[0, l : l + 1, :] = pltpu.roll(row, C, 1)[:, :C]
        return to_cols(row * total_m)

    def grad_z(l, dy, dx):
        n = POS // COLS
        return wide(par[10 + l], n) * (gy_ref[...] - wide(dy, n) - xhat[l] * wide(dx, n))

    def input_grad(l, gz):
        store_taps(gz, g9h, g9l, -1)
        first = mm(wb[l], g9h[...])
        return first[:C] + first[C:] + mm(wb[l, :C, :], g9l[...])

    sums_start(3, LAYERS)
    pair_back()
    sums_cross(LAYERS)
    gz = grad_z(3, *sums_end(3, LAYERS))
    zh[3], zl[3] = split(gz)
    gy = input_grad(3, gz) * slope[2]
    gy_ref[...] = gy
    row_2 = to_row(fold(gy), fold(gy * xhat[2]))
    gy = input_grad(2, wide(par[12], POS // COLS) * gy) * slope[1]
    row_1 = to_row(fold(gy), fold(gy * xhat[1]))
    payload = jnp.concatenate([row_2, row_1], axis=1)
    for phase in range(2):
        q_src[phase] = payload
        q_buf[phase, me[phase]] = payload
        spread(
            phase, q_src.at[phase], q_buf.at[phase], q_send.at[phase], q_recv.at[phase], True
        )
        (grad_start, grad_cross)[phase](3)
        settle(phase, q_buf.at[phase], q_recv.at[phase])
        payload = jnp.sum(q_buf[phase, pl.ds(0, groups[phase])], axis=0)
    row_2, row_1 = payload[:, :COLS], payload[:, COLS:]
    dy, dx = norms_done(2, row_2)
    settle(0, d_full, d_recv.at[2])
    factors = jnp.concatenate([d_full[i] for i in range(ga)], axis=0)
    moved = factors * jnp.concatenate([par[12] * dy, par[12] * dx], axis=0)
    row_1 = row_1 - jnp.sum(moved, axis=0, keepdims=True)
    gz = grad_z(2, dy, dx)
    zh[2], zl[2] = split(gz)
    gy_ref[...] = input_grad(2, gz) * slope[1]
    gz = grad_z(1, *norms_done(1, row_1))
    zh[1], zl[1] = split(gz)
    u_ref[...] = input_grad(1, gz)
    rnd = LAYERS + 1
    sums_start(0, rnd)
    grad_start(0, *split(gy_ref[...]))
    grad_start(2)
    grad_start(1)
    grad_back(3)
    sums_cross(rnd)
    grad_cross(0)
    grad_cross(2)
    grad_cross(1)
    settle(1, cx_buf, c_recv.at[1])
    fixed = jnp.sum(cx_buf[...], axis=0)
    dy, dx = sums_end(0, rnd)
    for k, tile in enumerate((dy, dx, par[10])):
        for q in range(nx * ny):
            trio[k, q] = tile[q * rows : (q + 1) * rows]

    def finish(part):
        dy_m, dx_m, k_m = [wide(trio[k, mine], LANES // COLS) for k in range(3)]
        return k_m * (part - fixed[rows:] * dy_m - fixed[:rows] * dx_m)

    grad_back(0, finish)
    grad_back(2)
    grad_back(1)
    gz = grad_z(0, dy, dx)
    for b in range(3):
        hi, lo = split(col_shift(gz, 1 if b == 0 else 0))
        for a in range(3):
            at = slice((3 * a + b) * C, (3 * a + b + 1) * C)
            g9h[at, :] = row_shift(hi, 1 if a == 0 else 0)
            g9l[at, :] = row_shift(lo, 1 if a == 0 else 0)
    u0 = mm(w0h[...], g9h[...]) + mm(w0l[...], g9h[...]) + mm(w0h[...], g9l[...])
    for s in range(SW):
        acc = jnp.zeros((2 * C, PILL), F32)
        for ph in range(4):
            hi, lo = split(u0[ph * C : (ph + 1) * C, s * PLANE : (s + 1) * PLANE])
            both = jnp.concatenate([hi, lo], axis=0)
            acc = acc + mm(both, hot[s, ph * PLANE : (ph + 1) * PLANE, :])
        pillar_out[s] = acc[:C] + acc[C:]

    for phase in range(2):
        settle(phase, p_buf.at[phase], p_send.at[phase])
        settle(phase, q_buf.at[phase], q_send.at[phase])
        for r in range(LAYERS + 2):
            settle(phase, s_buf.at[r, phase], s_send.at[r, phase])
    settle(0, d_buf, d_send.at[0])
    settle(1, dx_buf, d_send.at[1])
    settle(0, d_full, d_send.at[2])
    settle(0, c_buf, c_send.at[0])
    settle(1, cx_buf, c_send.at[1])
    for l in range(LAYERS):
        settle(0, rs_buf.at[l], g_send.at[l, 0])
        settle(1, x_buf.at[l], g_send.at[l, 1])
        settle(0, full.at[l], g_send.at[l, 2])
        settle(0, full.at[l], g_recv.at[l, 2])
        span = rows * C
        for i in range(ga):
            lanes = slice((i % (nx * ny)) * span, (i % (nx * ny) + 1) * span)
            first = (i // (nx * ny)) * (LANES // C)
            count = min(LANES // C, 9 - first)
            grads_out[first : first + count, l, lanes] = full[l, i, :count, :]


def deliver_kernel(*refs):
    *refs, sem = refs
    half = len(refs) // 2
    copies = [
        pltpu.make_async_copy(refs[k], refs[half + k], sem.at[k]) for k in range(half)
    ]
    for copy in copies:
        copy.start()
    for copy in copies:
        copy.wait()


def deliver(arrays):
    return pl.pallas_call(
        deliver_kernel,
        out_shape=tuple(jax.ShapeDtypeStruct(a.shape, a.dtype) for a in arrays),
        in_specs=[pl.BlockSpec(memory_space=pltpu.VMEM)] * len(arrays),
        out_specs=(pl.BlockSpec(memory_space=pl.ANY),) * len(arrays),
        scratch_shapes=[pltpu.SemaphoreType.DMA((len(arrays),))],
        compiler_params=pltpu.CompilerParams(vmem_limit_bytes=VLIM * 2**20),
    )(*arrays)


def solution(mesh, ny=NY, nz=NZ):
    nx = mesh.shape["rack"] // CORES
    ga, gb = CORES * nx * ny, nz
    gmax = max(ga, gb)
    rows = C // (nx * ny)

    def per_device(
        points, counts, cells, pfn_w, pfn_g, pfn_b, conv_w, bn_g, bn_b, cotangent
    ):
        vmem = pl.BlockSpec(memory_space=pltpu.VMEM)
        dma = pltpu.SemaphoreType.DMA
        out = pl.pallas_call(
            functools.partial(step_kernel, (nx, ny, nz)),
            out_shape=(
                jax.ShapeDtypeStruct((SW, C, ROWS, COLS), F32),
                jax.ShapeDtypeStruct((9, LAYERS, C * C), F32),
                jax.ShapeDtypeStruct((2, LAYERS, C), F32),
                jax.ShapeDtypeStruct((SW, C, PILL), F32),
            ),
            in_specs=[vmem] * 10,
            out_specs=(vmem,) * 4,
            scratch_shapes=[
                pltpu.VMEM((LAYERS, K9, POS), BF16),
                pltpu.VMEM((LAYERS, K9, POS), BF16),
                pltpu.VMEM((K9, POS), BF16),
                pltpu.VMEM((K9, POS), BF16),
                pltpu.VMEM((SW, 4 * PLANE, PILL), BF16),
                pltpu.VMEM((LAYERS, C, POS), F32),
                pltpu.VMEM((LAYERS, C, POS), F32),
                pltpu.VMEM((LAYERS, 2 * C, K9), BF16),
                pltpu.VMEM((LAYERS, 2 * C, K9), BF16),
                pltpu.VMEM((4 * C, K9), BF16),
                pltpu.VMEM((4 * C, K9), BF16),
                pltpu.VMEM((C, 5, LAYERS, COLS), F32),
                pltpu.VMEM((14, C, COLS), F32),
                pltpu.VMEM((10, C, COLS), F32),
                pltpu.VMEM((SW, C, PILL), F32),
                pltpu.VMEM((SW, C, PILL), F32),
                pltpu.VMEM((C, COLS), F32),
                pltpu.VMEM((C, POS), F32),
                pltpu.VMEM((C, POS), F32),
                pltpu.VMEM((2, 1, 2 * COLS), F32),
                pltpu.VMEM((2, gmax, 1, 2 * COLS), F32),
                pltpu.VMEM((LAYERS + 2, 2, 1, COLS), F32),
                pltpu.VMEM((LAYERS + 2, 2, gmax, 1, COLS), F32),
                pltpu.VMEM((LAYERS, ga, rows, LANES), F32),
                pltpu.VMEM((LAYERS, ga, rows, LANES), F32),
                pltpu.VMEM((LAYERS, rows, LANES), F32),
                pltpu.VMEM((LAYERS, gb, rows, LANES), F32),
                pltpu.VMEM((LAYERS, LANES // C, rows * C), F32),
                pltpu.VMEM((LAYERS, ga, LANES // C, rows * C), F32),
                pltpu.VMEM((ga, 2 * rows, LANES), F32),
                pltpu.VMEM((ga, 2 * rows, LANES), F32),
                pltpu.VMEM((2 * rows, LANES), F32),
                pltpu.VMEM((gb, 2 * rows, LANES), F32),
                pltpu.VMEM((3, ga // CORES, rows, COLS), F32),
                pltpu.VMEM((LAYERS, C, POS), BF16),
                pltpu.VMEM((LAYERS, C, POS), BF16),
                pltpu.VMEM((ga, 2 * C // ga, COLS), F32),
                pltpu.VMEM((ga, 2 * C // ga, COLS), F32),
                pltpu.VMEM((2 * C // ga, COLS), F32),
                pltpu.VMEM((gb, 2 * C // ga, COLS), F32),
                pltpu.VMEM((2 * C // ga, COLS), F32),
                pltpu.VMEM((ga, 2 * C // ga, COLS), F32),
                pltpu.VMEM((2, 1, 2 * COLS), F32),
                pltpu.VMEM((2, gmax, 1, 2 * COLS), F32),
                dma((2,)),
                dma((2,)),
                dma((3,)),
                dma((3,)),
                dma((2,)),
                dma((2,)),
                dma((2,)),
                dma((2,)),
                dma((LAYERS + 2, 2)),
                dma((LAYERS + 2, 2)),
                dma((LAYERS, 3)),
                dma((LAYERS, 3)),
            ],
            compiler_params=pltpu.CompilerParams(
                collective_id=0, has_side_effects=True, vmem_limit_bytes=VLIM * 2**20
            ),
        )(
            points,
            counts,
            cells,
            pfn_w,
            pfn_g.reshape(1, C),
            pfn_b.reshape(1, C),
            conv_w.transpose(1, 0, 2),
            bn_g,
            bn_b,
            cotangent,
        )
        features, grads, norm_grads, pillar_grad = deliver(out)
        return features, grads.transpose(1, 0, 2), norm_grads, pillar_grad

    split_all = ("rack", "chip")
    return jax.shard_map(
        per_device,
        mesh=mesh,
        in_specs=(
            P(split_all, None, None, None),
            P(split_all, None),
            P(split_all, None),
            P(),
            P(),
            P(),
            P(),
            P(),
            P(),
            P(split_all, None, None, None),
        ),
        out_specs=(
            P(split_all, None, None, None),
            P(),
            P(),
            P(split_all, None, None),
        ),
        check_vma=False,
    )
```
